128 devices in a mesh: aa: 8 (over x, core), ba: 16 (over z, y).
Axes of the slice: x: 4, y: 4, z: 4, core: 2. Of those that a mesh axis runs over, the one named last changes fastest.
Arguments:
- positions: float32 [3, 65536], P(None, ('aa', 'ba')), may hold values from -1.5 to 1.5
- forces: float32 [3, 65536], P(None, ('aa', 'ba')), may hold values from -3 to 3
- tension: float32 [65536], P(('aa', 'ba')), may hold values from -6 to 6
- node_slot: int32 [65536], P(('aa', 'ba')), may hold values from 0 to 65535, as said below
- leaf_local: float32 [2048, 3, 128], P(('aa', 'ba')), may hold values from -24 to 24
- parent_local: float32 [256, 3, 128], P(('aa', 'ba')), may hold values from -24 to 24
- l2l_maps: float32 [8, 384, 384], replicated, may hold values from -0.3125 to 0.3125
- leaf_parent: int32 [2048], P(('aa', 'ba')), may hold values from 0 to 255, as said below
- leaf_octant: int32 [2048], P(('aa', 'ba')), may hold values from 0 to 7
- near_list: int32 [2048, 27], P(('aa', 'ba')), may hold values from 0 to 2047, as said below
- blocks: float32 [1024, 256, 256], P(('aa', 'ba')), may hold values from -0.375 to 0.375
Outputs:
- result: float32 [1024, 256], P(('aa', 'ba'))
The draws below stay inside these ranges and needn't reach their ends.
Inputs may be any that keep to these rules, and one draw needn't show every extreme that they name: `node_slot`: A permutation. Of the nodes of one device (512 in a row), at most 16 have slots in the range of any one device (512 consecutive slots), and some pair of devices reaches 16. Every device has nodes in the ranges of the devices just before and just after it, counted round. `leaf_parent`: the parent of a leaf of device d lies among parents 2 * (d - 1) to 2 * (d + 2) - 1. `near_list`: each row holds 27 different leaves, the first the leaf itself, all within 128 leaves of it.
All inputs are finite; a program needn't handle non-finite values. Where the reference program divides by a largest or mean magnitude, that divisor is 1e-20 or more.
Results may differ from the reference program's by a relative error of at most 0.00012.
Values sent between devices are 32-bit elements; how exact they have to be, the bound alone decides.
No kernel may reach another device: no remote copies, remote signals or barrier semaphores. Data moves between devices by JAX's collectives and lax.ppermute only.
A program may use at most 64 MiB of HBM per device.

```python
import jax
import jax.numpy as jnp
from jax import lax

NPF = 64
BLK = 256
NODE_DEV = 512
FIBERS = 1024
NODES = 65536
LPTS = 32
LEAF_DEV = 16
LEAVES = 2048
PAR_DEV = 2
PARENTS = 256
NEQ = 128
NEAR = 27
REACH = 8
MOST = 4
PIECE = 4


def draw_node_slot(key, part):
    devices = NODES // NODE_DEV
    groups = devices // MOST
    bins_drawn = jax.random.randint(jax.random.fold_in(key, 11), (groups, MOST), 0, MOST)
    bins_drawn = bins_drawn.at[0].set(0)
    bins_drawn = bins_drawn.at[1].set(jnp.arange(MOST))
    counts = jnp.sum((bins_drawn[:, :, None] == jnp.arange(MOST)[None, None, :]).astype(jnp.int32), axis=1).reshape(-1)
    values = jnp.arange(devices)
    pinned = (values == devices // 2) | (values == 1) | (values == devices - 1)
    score = jax.random.permutation(jax.random.fold_in(key, 12), devices) + devices * pinned.astype(jnp.int32)
    remaining = jnp.argsort(score, stable=True)[:devices - 3]
    other_spots = jnp.array([spot for spot in range(devices) if spot not in (0, MOST, MOST + 1)], jnp.int32)
    shuffled = jnp.zeros((devices,), jnp.int32).at[other_spots].set(remaining.astype(jnp.int32))
    shuffled = shuffled.at[jnp.array([0, MOST, MOST + 1], jnp.int32)].set(jnp.array([devices // 2, 1, devices - 1], jnp.int32))
    by_offset = jnp.zeros((devices,), jnp.int32).at[shuffled].set(counts)
    cumulative = jnp.cumsum(by_offset)
    offset_of = jnp.searchsorted(cumulative, jnp.arange(devices), side='right').astype(jnp.int32)

    def shuffle_one(subkey):
        return jax.random.permutation(subkey, devices)
    send_order = jax.vmap(shuffle_one)(jax.random.split(jax.random.fold_in(key, 13), devices))
    recv_order = jax.vmap(shuffle_one)(jax.random.split(jax.random.fold_in(key, 14), devices))
    source = jnp.arange(devices)[:, None]
    target = (source + offset_of[send_order]) % devices
    placed = recv_order[target, send_order]
    slot_ids = target[:, :, None] * NODE_DEV + placed[:, :, None] * PIECE + jnp.arange(PIECE)[None, None, :]
    return slot_ids.reshape(NODES).astype(jnp.int32)


def draw_leaf_parent(key, part):
    leaf_ids = jnp.arange(LEAVES)
    device = leaf_ids // LEAF_DEV
    inner = leaf_ids % LEAF_DEV
    first_parent = device * PAR_DEV + inner * PAR_DEV // LEAF_DEV
    jitter = jax.random.randint(jax.random.fold_in(key, 21), (LEAVES,), -2, 3)
    return jnp.clip(first_parent + jitter, 0, PARENTS - 1).astype(jnp.int32)


def draw_near_list(key, part):
    span = REACH * LEAF_DEV

    def pick_one(subkey):
        return jax.random.permutation(subkey, span)[:NEAR - 1] + 1
    distance = jax.vmap(pick_one)(jax.random.split(jax.random.fold_in(key, 31), LEAVES))
    direction = 2 * jax.random.randint(jax.random.fold_in(key, 32), (LEAVES, NEAR - 1), 0, 2) - 1
    leaf_ids = jnp.arange(LEAVES)[:, None]
    forward = leaf_ids + direction * distance
    inside = (forward >= 0) & (forward < LEAVES)
    chosen = jnp.where(inside, forward, leaf_ids - direction * distance)
    return jnp.concatenate([leaf_ids, chosen], axis=1).astype(jnp.int32)


def touch_ends(drawn, own_key, least, largest):
    shape = drawn.shape
    place = [jax.random.randint(jax.random.fold_in(own_key, axis), (), 0, shape[axis]) for axis in range(len(shape))]
    drawn = drawn.at[tuple(place)].set(least)
    longest = shape.index(max(shape))
    place[longest] = (place[longest] + 1) % shape[longest]
    return drawn.at[tuple(place)].set(largest)


def block_scale(own_key, shape, cuts, least, high):
    level, own = 1.0, jax.random.fold_in(own_key, 6)
    for dim, blocks in cuts:
        steps = jnp.exp(jax.random.uniform(jax.random.fold_in(own, dim), (blocks,), jnp.float32, least / len(cuts), high / len(cuts)))
        level = level * jnp.repeat(steps, shape[dim] // blocks).reshape([-1 if axis == dim else 1 for axis in range(len(shape))])
    return level


def bell_draw(key, shape, width, bound, cuts=(), held_as=jnp.bfloat16):
    values = jax.random.normal(key, shape, jnp.float32) * width
    if len(cuts) > 0:
        values = block_scale(key, shape, cuts, -0.22, 0.18) * values
    return jnp.clip(values, min=-bound, max=bound).astype(held_as)


def setup_inputs(seed: int = 0) -> dict:
    streams_of = jax.random.split(jax.random.key(seed), 12)
    return {
        "positions": bell_draw(streams_of[0], (3, NODES), 0.25, 1.5, ((1, 128),), jnp.float32),
        "forces": bell_draw(streams_of[1], (3, NODES), 0.5, 3.0, ((1, 128),), jnp.float32),
        "tension": bell_draw(streams_of[2], (NODES,), 1.0, 6.0, ((0, 128),), jnp.float32),
        "node_slot": draw_node_slot(jax.random.fold_in(streams_of[11], 71), 0),
        "leaf_local": bell_draw(streams_of[4], (LEAVES, 3, NEQ), 4.0, 24.0, ((0, 128),), jnp.float32),
        "parent_local": bell_draw(streams_of[5], (PARENTS, 3, NEQ), 4.0, 24.0, ((0, 128),), jnp.float32),
        "l2l_maps": bell_draw(streams_of[6], (8, 3 * NEQ, 3 * NEQ), (3 * NEQ) ** -0.5, 0.3125, (), jnp.float32),
        "leaf_parent": draw_leaf_parent(jax.random.fold_in(streams_of[11], 71), 0),
        "leaf_octant": touch_ends(jax.random.randint(streams_of[8], (LEAVES,), 0, 8), jax.random.fold_in(streams_of[8], 1), 0, 7).astype(jnp.int32),
        "near_list": draw_near_list(jax.random.fold_in(streams_of[11], 71), 0),
        "blocks": bell_draw(streams_of[10], (FIBERS, BLK, BLK), BLK ** -0.5, 0.375, ((0, 128),), jnp.float32),
    }


exact_products = lax.Precision.HIGHEST
softening = 0.05
box_margin = 0.05
shell_radius = 2.95
golden_angle = 2.399963229728653
eight_pi = 25.132741228718345
leaf_group = 16

def surface(amount):
    indices = jnp.arange(amount).astype(jnp.float32) + 0.5
    height = 1.0 - 2.0 * indices / amount
    radius = jnp.sqrt(jnp.maximum(1.0 - height * height, 0.0))
    azimuth = indices * golden_angle
    spread = jnp.stack([radius * jnp.cos(azimuth), radius * jnp.sin(azimuth), height])
    return spread / lax.optimization_barrier(jnp.max(jnp.abs(spread), axis=0, keepdims=True))

def leaf_velocity(targets, sources, density, shell_points):
    center = lax.optimization_barrier(jnp.mean(targets, axis=2, keepdims=True))
    half_width = lax.optimization_barrier(jnp.max(jnp.abs(targets - center), axis=(1, 2), keepdims=True)) + box_margin
    equivalent = center + shell_radius * half_width * shell_points[None, :, :]
    separation = targets[:, :, :, None] - equivalent[:, :, None, :]
    inverse = 1.0 / jnp.sqrt(lax.optimization_barrier(jnp.sum(separation * separation, axis=1)))
    along = jnp.einsum('bkpq,bkq->bpq', separation, density, precision=exact_products)
    far_field = jnp.einsum('bpq,bkq->bkp', inverse, density, precision=exact_products)
    far_field = far_field + jnp.einsum('bkpq,bpq->bkp', separation, along * inverse ** 3, precision=exact_products)
    near_gap = targets[:, :, :, None] - sources[:, 0:3, None, :]
    distance_sq = lax.optimization_barrier(jnp.sum(near_gap * near_gap, axis=1))
    weight = (distance_sq + softening ** 2) ** (-1.5)
    strengths = sources[:, 3:6]
    projection = jnp.einsum('bkps,bks->bps', near_gap, strengths, precision=exact_products)
    near_field = jnp.einsum('bps,bks->bkp', (distance_sq + 2.0 * softening ** 2) * weight, strengths, precision=exact_products)
    near_field = near_field + jnp.einsum('bkps,bps->bkp', near_gap, projection * weight, precision=exact_products)
    return (far_field + near_field) / eight_pi

def reference(positions, forces, tension, node_slot, leaf_local, parent_local, l2l_maps, leaf_parent, leaf_octant, near_list, blocks):
    payload = jnp.concatenate([positions, forces], axis=0)
    tree_data = jnp.zeros((6, NODES), jnp.float32).at[:, node_slot].set(payload)
    leaf_data = tree_data.reshape(6, LEAVES, LPTS).transpose(1, 0, 2)
    flat_parent = parent_local[leaf_parent].reshape(LEAVES, 3 * NEQ)
    translated = jnp.zeros((LEAVES, 3 * NEQ), jnp.float32)
    for octant in range(8):
        image = jnp.dot(flat_parent, l2l_maps[octant].T, precision=exact_products)
        translated = jnp.where((leaf_octant == octant)[:, None], image, translated)
    density = leaf_local + translated.reshape(LEAVES, 3, NEQ)
    shell_points = surface(NEQ)
    groups = LEAVES // leaf_group

    def one_group(items):
        targets, near_rows, dens = items
        sources = leaf_data[near_rows].transpose(0, 2, 1, 3).reshape(leaf_group, 6, NEAR * LPTS)
        return leaf_velocity(targets, sources, dens, shell_points)
    velocity = lax.map(one_group, (leaf_data[:, 0:3].reshape(groups, leaf_group, 3, LPTS), near_list.reshape(groups, leaf_group, NEAR), density.reshape(groups, leaf_group, 3, NEQ)))
    velocity = velocity.reshape(LEAVES, 3, LPTS).transpose(1, 0, 2).reshape(3, NODES)
    fiber_velocity = velocity[:, node_slot]
    stacked = fiber_velocity.reshape(3, FIBERS, NPF).transpose(1, 0, 2).reshape(FIBERS, 3 * NPF)
    vector = jnp.concatenate([stacked, tension.reshape(FIBERS, NPF)], axis=1)
    return jnp.einsum('fij,fj->fi', blocks, vector, precision=exact_products)
```

```python
import jax
import jax.numpy as jnp
import numpy as np
from jax import lax
from jax.experimental import pallas as pl
from jax.experimental.pallas import tpu as pltpu
from jax.sharding import PartitionSpec as P

DEVICES = 128
NODES = 512
CAP = 16
REACH = 8
SPAN = 2 * REACH + 1
LEAVES = 16
LPTS = 32
NEAR = 27
NEQ = 128
LANES = LEAVES * LPTS
WORDS = 7 * SPAN * CAP
CHUNKS = 15
EPS2 = 0.05**2
MARGIN = 0.05
SHELL = 2.95
GOLDEN = 2.399963229728653
EIGHT_PI = 25.132741228718345
AXES = ("aa", "ba")
HIGHEST = lax.Precision.HIGHEST
F32, BF16 = jnp.float32, jnp.bfloat16
NT = (((1,), (1,)), ((), ()))
NN = (((1,), (0,)), ((), ()))


def iota(shape, dim):
    return lax.broadcasted_iota(jnp.int32, shape, dim)


def three(x):
    high = x.astype(BF16).astype(F32)
    rest = x - high
    middle = rest.astype(BF16).astype(F32)
    return high, middle, rest - middle


def two(x):
    high = x.astype(BF16)
    return high, (x - high.astype(F32)).astype(BF16)


def dot(a, b, dims):
    return lax.dot_general(a, b, dims, preferred_element_type=F32)


def thirds(x, rows):
    return x[:rows] + x[rows : 2 * rows] + x[2 * rows :]


def shell_table():
    q = np.arange(NEQ, dtype=np.float32) + np.float32(0.5)
    h = (np.float32(1.0) - np.float32(2.0) * q / np.float32(NEQ)).astype(np.float32)
    radius = np.sqrt(np.maximum(np.float32(1.0) - h * h, 0)).astype(np.float32)
    angle = (q * np.float32(GOLDEN)).astype(np.float32)
    w = np.stack([radius * np.cos(angle), radius * np.sin(angle), h]).astype(np.float32)
    s = w / np.max(np.abs(w), axis=0, keepdims=True)
    table = np.zeros((3, LPTS, LANES), np.float32)
    for g in range(NEQ // LPTS):
        table[:, :, NEAR + g :: LPTS] = s[:, g * LPTS : (g + 1) * LPTS, None]
    return table.reshape(3 * LPTS, LANES)


def owner_hot(slot):
    return (iota((DEVICES, NODES), 0) == (slot >> 9)).astype(F32)


def pack_kernel(pos_ref, force_ref, slot_ref, message_ref, rank_ref, rows_ref):
    slot = slot_ref[...]
    hot = owner_hot(slot)
    hot_b = hot.astype(BF16)
    before = (iota((NODES, NODES), 0) < iota((NODES, NODES), 1)).astype(F32).astype(BF16)
    rank = jnp.sum(hot * dot(hot_b, before, NN), axis=0, keepdims=True)
    rank_ref[...] = rank
    here = iota((CAP, NODES), 0).astype(F32) == rank
    within = (slot & (NODES - 1)).astype(F32) + 1.0
    payload = [pos_ref[c : c + 1, :] for c in range(3)]
    payload += [force_ref[c : c + 1, :] for c in range(3)] + [within]
    spread = jnp.concatenate([jnp.where(here, row, 0.0) for row in payload], axis=0)
    terms = jnp.concatenate(three(spread), axis=0).astype(BF16)
    buckets = thirds(dot(terms, hot_b, NT), 7 * CAP)
    rows_ref[WORDS:, :] = jnp.zeros((CHUNKS * 128 - WORDS, DEVICES), F32)
    for d in range(SPAN):
        shift = (REACH - d) % DEVICES
        moved = pltpu.roll(buckets, shift, 1) if shift else buckets
        for c in range(7):
            at = c * SPAN * CAP + d * CAP
            rows_ref[at : at + CAP, :] = moved[c * CAP : (c + 1) * CAP, :]
    for i in range(CHUNKS):
        message_ref[pl.ds(i, DEVICES, stride=CHUNKS), :] = rows_ref[i * 128 : (i + 1) * 128, :].T


def density_kernel(
    parent_ref, octant_ref, before_ref, own_ref, after_ref, local_ref, maps_ref, out_ref,
    six_ref, picked_ref, total_ref,
):
    o = pl.program_id(0)
    wide = 3 * NEQ

    @pl.when(o == 0)
    def _():
        for j in range(6):
            source = (before_ref, own_ref, after_ref)[j // 2]
            for c in range(3):
                six_ref[c * 8 + j : c * 8 + j + 1, :] = source[j % 2, c : c + 1, :]
        for l in range(LEAVES):
            for c in range(3):
                picked_ref[l : l + 1, c * NEQ : (c + 1) * NEQ] = six_ref[
                    pl.ds(c * 8 + parent_ref[l], 1), :
                ]
        total_ref[...] = jnp.zeros_like(total_ref)

    lane = iota((1, 2 * LEAVES), 1) % LEAVES
    octants = jnp.zeros((1, 2 * LEAVES), jnp.int32)
    for l in range(LEAVES):
        octants = jnp.where(lane == l, octant_ref[l], octants)
    weights = jnp.concatenate(two(picked_ref[...]), axis=0)
    high, low = two(maps_ref[0])
    image = dot(high, weights, NT) + dot(low, weights, NT)
    total_ref[...] += jnp.where(octants == o, image, 0.0)

    @pl.when(o == 7)
    def _():
        total = total_ref[...]
        moved = total[:, :LEAVES] + total[:, LEAVES:]
        lane = iota((LEAVES, LANES), 1)
        row = iota((LEAVES, LANES), 0)
        pieces = []
        for c in range(3):
            local = jnp.concatenate(
                [local_ref[:, c, :], jnp.zeros((NEQ - LEAVES, NEQ), F32)], axis=0
            ).T[:, :LEAVES]
            pieces.append(local + moved[c * NEQ : (c + 1) * NEQ])
        placed = jnp.zeros((3 * LPTS, LANES), F32)
        for g in range(NEQ // LPTS):
            group = jnp.concatenate([p[g * LPTS : (g + 1) * LPTS] for p in pieces], axis=0)
            place = (lane == row * LPTS + NEAR + g).astype(F32)
            placed = placed + lax.dot_general(
                group, place, NN, precision=HIGHEST, preferred_element_type=F32
            )
        out_ref[...] = placed


def field_kernel(
    arrived_ref, near_ref, density_ref, shell_ref, out_ref,
    turned_ref, tree_ref, source_ref, target_ref, partial_ref, back_ref,
):
    entries = SPAN * CAP
    turned = []
    for i in range(CHUNKS):
        turned.append(arrived_ref[pl.ds(i, DEVICES, stride=CHUNKS), :].T)
    turned = jnp.concatenate(turned, axis=0)
    for c in range(7):
        turned_ref[pl.ds(c, entries, stride=8), :] = turned[c * entries : (c + 1) * entries, :]
    turned_ref[pl.ds(7, entries, stride=8), :] = jnp.zeros((entries, DEVICES), F32)
    tree_ref[SPAN * 32 :, :] = jnp.zeros((1024 - SPAN * 32, 128), F32)
    low_row = iota((128, 128), 0)

    def place(d, carry):
        lows, values = [], []
        for r in range(CAP):
            entry = turned_ref[pl.ds(pl.multiple_of((d * CAP + r) * 8, 8), 8), :]
            slot = entry[6:7, :].astype(jnp.int32) - 1
            lows.append((low_row == (slot & 127)).astype(F32).astype(BF16))
            high = slot >> 7
            parts = three(entry)
            values.append(
                jnp.concatenate(
                    [jnp.where(high == h, part, 0.0) for part in parts for h in range(4)], axis=0
                ).astype(BF16)
            )
        placed = dot(jnp.concatenate(values, axis=1), jnp.concatenate(lows, axis=1), NT)
        tree_ref[pl.ds(pl.multiple_of(d * 32, 32), 32), :] = thirds(placed, 32)
        return carry

    lax.fori_loop(0, SPAN, place, 0)

    terms = [[], [], []]
    for c in range(6):
        turned_c = tree_ref[pl.ds(c, 128, stride=8), :].T
        for s, part in enumerate(three(turned_c)):
            part = part.astype(BF16)
            terms[s].append(
                jnp.concatenate([part[w * LPTS : (w + 1) * LPTS] for w in range(4)], axis=1)
            )
    everything = jnp.concatenate([t for s in range(3) for t in terms[s]], axis=0)
    positions = jnp.concatenate([t for s in range(3) for t in terms[s][:3]], axis=0)
    leaf_row = iota((128, LANES), 0)

    def hot(leaf):
        quarter, row = leaf & 3, leaf >> 2
        return jnp.concatenate(
            [
                (leaf_row == jnp.where(quarter == w, row, -1)).astype(F32).astype(BF16)
                for w in range(4)
            ],
            axis=0,
        )

    lane = iota((1, LANES), 1)
    gathered = thirds(dot(everything, hot(near_ref[...]), NN), 6 * LPTS)
    targets = thirds(dot(positions, hot(lane // LPTS + REACH * LEAVES), NN), 3 * LPTS)
    for k in range(LANES // 128):
        target_ref[k * 96 : (k + 1) * 96, :] = targets[:, k * 128 : (k + 1) * 128]
    axes = [targets[c * LPTS : (c + 1) * LPTS] for c in range(3)]
    centers = [jnp.sum(a, axis=0, keepdims=True) * (1.0 / LPTS) for a in axes]
    half = jnp.maximum(
        jnp.maximum(
            jnp.max(jnp.abs(axes[0] - centers[0]), axis=0, keepdims=True),
            jnp.max(jnp.abs(axes[1] - centers[1]), axis=0, keepdims=True),
        ),
        jnp.max(jnp.abs(axes[2] - centers[2]), axis=0, keepdims=True),
    ) + MARGIN
    spot = lane % LPTS
    far = (spot >= NEAR) & (spot < NEAR + NEQ // LPTS)
    for c in range(3):
        rows = slice(c * LPTS, (c + 1) * LPTS)
        shell = jnp.where(far, centers[c], 0.0) + (SHELL * half) * shell_ref[rows, :]
        source_ref[rows, :] = gathered[rows, :] + shell
    source_ref[3 * LPTS :, :] = gathered[3 * LPTS :, :] + density_ref[...]

    soft = jnp.where(far, 0.0, EPS2)
    for chunk in range(LANES // 128):
        lanes = slice(chunk * 128, (chunk + 1) * 128)
        soft_c = soft[:, lanes]

        def step(p, carry):
            aim = [target_ref[pl.ds(chunk * 96 + c * LPTS + p, 1), :] for c in range(3)]
            sums = None
            for g in range(LPTS // 8):
                at = [source_ref[c * LPTS + g * 8 : c * LPTS + g * 8 + 8, lanes] for c in range(6)]
                gap = [aim[c] - at[c] for c in range(3)]
                square = gap[0] * gap[0] + gap[1] * gap[1] + gap[2] * gap[2] + soft_c
                inverse = lax.rsqrt(square)
                cube = inverse * inverse * inverse
                along = (gap[0] * at[3] + gap[1] * at[4] + gap[2] * at[5]) * cube
                plain = (square + soft_c) * cube
                new = [plain * at[3 + c] + gap[c] * along for c in range(3)]
                sums = new if sums is None else [a + b for a, b in zip(sums, new)]
            for c in range(3):
                partial_ref[pl.ds(chunk * 96 + c * LPTS + p, 1), :] = jnp.sum(
                    sums[c], axis=0, keepdims=True
                )
            return carry

        lax.fori_loop(0, LPTS, step, 0, unroll=2)

    same = (iota((LEAVES, LANES), 1) // LPTS == iota((LEAVES, LANES), 0)).astype(F32)
    partial = jnp.concatenate([partial_ref[k * 96 : (k + 1) * 96, :] for k in range(4)], axis=1)
    by_leaf = [
        lax.dot_general(
            same, partial[c * LPTS : (c + 1) * LPTS, :], NT, precision=HIGHEST,
            preferred_element_type=F32,
        )
        for c in range(3)
    ]
    velocity = jnp.concatenate(by_leaf, axis=0) * (1.0 / EIGHT_PI)
    velocity = jnp.concatenate(three(velocity), axis=0).astype(BF16)
    node_row = iota((LPTS, DEVICES), 0)
    leaf_of = iota((LEAVES, DEVICES), 0)
    back_ref[...] = jnp.zeros_like(back_ref)
    slots, hots = [], []
    for r in range(CAP):
        entry = turned_ref[(REACH * CAP + r) * 8 : (REACH * CAP + r) * 8 + 8, :]
        slot = entry[6:7, :].astype(jnp.int32) - 1
        slots.append(slot)
        hots.append((node_row == (slot & (LPTS - 1))).astype(F32).astype(BF16))
    picked = thirds(dot(velocity, jnp.concatenate(hots, axis=1), NN), 3 * LEAVES)
    for r in range(CAP):
        mine = leaf_of == (slots[r] >> 5)
        for c in range(3):
            piece = picked[c * LEAVES : (c + 1) * LEAVES, r * 128 : (r + 1) * 128]
            back_ref[c * CAP + r : c * CAP + r + 1, :] = jnp.sum(
                jnp.where(mine, piece, 0.0), axis=0, keepdims=True
            )
    out_ref[...] = back_ref[...].T


def fiber_kernel(arrived_ref, slot_ref, rank_ref, tension_ref, blocks_ref, out_ref, vector_ref):
    hot = owner_hot(slot_ref[...]).astype(BF16)
    words = arrived_ref[...].T[: 3 * CAP]
    terms = jnp.concatenate(three(words), axis=0).astype(BF16)
    picked = thirds(dot(terms, hot, NN), 3 * CAP)
    here = iota((CAP, NODES), 0).astype(F32) == rank_ref[...]
    rows = [
        jnp.sum(jnp.where(here, picked[c * CAP : (c + 1) * CAP], 0.0), axis=0, keepdims=True)
        for c in range(3)
    ] + [tension_ref[...]]
    first = iota((1, 128), 1) < 64
    for pair in range(NODES // 128):
        cut = [row[:, pair * 128 : (pair + 1) * 128] for row in rows]
        swapped = [pltpu.roll(row, 64, 1) for row in cut]
        for k in range(2):
            a, b = cut[2 * k], cut[2 * k + 1]
            sa, sb = swapped[2 * k], swapped[2 * k + 1]
            lanes = slice(k * 128, (k + 1) * 128)
            vector_ref[2 * pair : 2 * pair + 1, lanes] = jnp.where(first, a, sb)
            vector_ref[2 * pair + 1 : 2 * pair + 2, lanes] = jnp.where(first, sa, b)
    vector = jnp.concatenate(two(vector_ref[...]), axis=0)
    row = iota((16, 256), 0) % 8
    total = jnp.zeros((16, 256), F32)
    for i in range(8):
        high, low = two(blocks_ref[i])
        image = dot(vector, high, NT) + dot(vector, low, NT)
        total = jnp.where(row == i, image, total)
    out_ref[...] = total[:8] + total[8:]


def shape(*dims):
    return jax.ShapeDtypeStruct(dims, F32)


def shifted(value, by):
    return lax.ppermute(value, AXES, [(i, (i + by) % DEVICES) for i in range(DEVICES)])


def exchange(rows):
    return lax.all_to_all(rows.reshape(-1), AXES, 0, 0, tiled=True).reshape(rows.shape)


def local(
    positions, forces, tension, node_slot, leaf_local, parent_local, l2l_maps, leaf_parent,
    leaf_octant, near_list, blocks,
):
    device = lax.axis_index("aa") * lax.axis_size("ba") + lax.axis_index("ba")
    slot = node_slot.reshape(1, NODES)
    from_before = shifted(parent_local, 1)
    from_after = shifted(parent_local, -1)
    message, rank = pl.pallas_call(
        pack_kernel,
        out_shape=(shape(CHUNKS * 128, 128), shape(1, NODES)),
        scratch_shapes=[pltpu.VMEM((CHUNKS * 128, DEVICES), F32)],
        cost_estimate=pl.CostEstimate(flops=10**8, bytes_accessed=10**6, transcendentals=0),
        name="pack",
    )(positions, forces, slot)
    arrived = exchange(message)

    vmem = pl.BlockSpec(memory_space=pltpu.VMEM)
    smem = pl.BlockSpec(memory_space=pltpu.SMEM)
    density = pl.pallas_call(
        density_kernel,
        grid=(8,),
        out_shape=shape(3 * LPTS, LANES),
        in_specs=[smem, smem, vmem, vmem, vmem, vmem, pl.BlockSpec((1, 384, 384), lambda o: (o, 0, 0))],
        out_specs=pl.BlockSpec((3 * LPTS, LANES), lambda o: (0, 0)),
        scratch_shapes=[
            pltpu.VMEM((24, NEQ), F32),
            pltpu.VMEM((LEAVES, 3 * NEQ), F32),
            pltpu.VMEM((3 * NEQ, 2 * LEAVES), F32),
        ],
        cost_estimate=pl.CostEstimate(flops=10**9, bytes_accessed=5 * 10**6, transcendentals=0),
        name="density",
    )(
        leaf_parent - 2 * (device - 1), leaf_octant, from_before, parent_local, from_after,
        leaf_local, l2l_maps,
    )
    near = jnp.pad(
        near_list - LEAVES * (device - REACH), ((0, 0), (0, LPTS - NEAR)), constant_values=-1
    ).reshape(1, LANES)

    back = pl.pallas_call(
        field_kernel,
        out_shape=shape(DEVICES, 128),
        scratch_shapes=[
            pltpu.VMEM((SPAN * CAP * 8, DEVICES), F32),
            pltpu.VMEM((1024, 128), F32),
            pltpu.VMEM((6 * LPTS, LANES), F32),
            pltpu.VMEM((12 * LPTS, 128), F32),
            pltpu.VMEM((12 * LPTS, 128), F32),
            pltpu.VMEM((128, DEVICES), F32),
        ],
        cost_estimate=pl.CostEstimate(flops=10**9, bytes_accessed=2 * 10**6, transcendentals=0),
        name="field",
    )(arrived, near, density, jnp.asarray(shell_table()))
    returned = exchange(back)
    return pl.pallas_call(
        fiber_kernel,
        out_shape=shape(8, 256),
        scratch_shapes=[pltpu.VMEM((8, 256), F32)],
        cost_estimate=pl.CostEstimate(flops=10**8, bytes_accessed=2 * 10**6, transcendentals=0),
        name="fiber",
    )(returned, slot, rank, tension.reshape(1, NODES), blocks)


def solution(mesh):
    both = ("aa", "ba")
    in_specs = (
        P(None, both), P(None, both), P(both), P(both), P(both, None, None), P(both, None, None),
        P(), P(both), P(both), P(both, None), P(both, None, None),
    )
    return jax.shard_map(
        local, mesh=mesh, in_specs=in_specs, out_specs=P(both, None), check_vma=False
    )
```

```python
import jax
import jax.numpy as jnp
import numpy as np
from jax import lax
from jax.experimental import pallas as pl
from jax.experimental.pallas import tpu as pltpu
from jax.sharding import PartitionSpec as P

DEVICES = 128
NODES = 512
CAP = 16
REACH = 8
SPAN = 2 * REACH + 1
LEAVES = 16
LPTS = 32
NEAR = 27
NEQ = 128
LANES = LEAVES * LPTS
WORDS = 7 * SPAN * CAP
CHUNKS = 15
MAPS_GRANT = 8
EPS2 = 0.05**2
MARGIN = 0.05
SHELL = 2.95
GOLDEN = 2.399963229728653
EIGHT_PI = 25.132741228718345
AXES = ("aa", "ba")
HIGHEST = lax.Precision.HIGHEST
F32, BF16 = jnp.float32, jnp.bfloat16
NT = (((1,), (1,)), ((), ()))
NN = (((1,), (0,)), ((), ()))


def iota(shape, dim):
    return lax.broadcasted_iota(jnp.int32, shape, dim)


def three(x):
    high = x.astype(BF16).astype(F32)
    rest = x - high
    middle = rest.astype(BF16).astype(F32)
    return high, middle, rest - middle


def two(x):
    high = x.astype(BF16)
    return high, (x - high.astype(F32)).astype(BF16)


def dot(a, b, dims):
    return lax.dot_general(a, b, dims, preferred_element_type=F32)


def thirds(x, rows):
    return x[:rows] + x[rows : 2 * rows] + x[2 * rows :]


def shell_table():
    q = np.arange(NEQ, dtype=np.float32) + np.float32(0.5)
    h = (np.float32(1.0) - np.float32(2.0) * q / np.float32(NEQ)).astype(np.float32)
    radius = np.sqrt(np.maximum(np.float32(1.0) - h * h, 0)).astype(np.float32)
    angle = (q * np.float32(GOLDEN)).astype(np.float32)
    w = np.stack([radius * np.cos(angle), radius * np.sin(angle), h]).astype(np.float32)
    s = w / np.max(np.abs(w), axis=0, keepdims=True)
    table = np.zeros((3, LPTS, LANES), np.float32)
    for g in range(NEQ // LPTS):
        table[:, :, NEAR + g :: LPTS] = s[:, g * LPTS : (g + 1) * LPTS, None]
    return table.reshape(3 * LPTS, LANES)


def device_index():
    return lax.axis_index("aa") * 16 + lax.axis_index("ba")


def owner_hot(slot):
    return (iota((DEVICES, NODES), 0) == (slot >> 9)).astype(F32)


def pack_kernel(pos_ref, force_ref, slot_ref, message_ref, rank_ref, rows_ref):
    slot = slot_ref[...]
    hot = owner_hot(slot)
    hot_b = hot.astype(BF16)
    before = (iota((NODES, NODES), 0) < iota((NODES, NODES), 1)).astype(F32).astype(BF16)
    rank = jnp.sum(hot * dot(hot_b, before, NN), axis=0, keepdims=True)
    rank_ref[...] = rank
    here = iota((CAP, NODES), 0).astype(F32) == rank
    within = (slot & (NODES - 1)).astype(F32) + 1.0
    payload = [pos_ref[c : c + 1, :] for c in range(3)]
    payload += [force_ref[c : c + 1, :] for c in range(3)] + [within]
    spread = jnp.concatenate([jnp.where(here, row, 0.0) for row in payload], axis=0)
    terms = jnp.concatenate(three(spread), axis=0).astype(BF16)
    buckets = thirds(dot(terms, hot_b, NT), 7 * CAP)
    rows_ref[WORDS:, :] = jnp.zeros((CHUNKS * 128 - WORDS, DEVICES), F32)
    for d in range(SPAN):
        shift = (REACH - d) % DEVICES
        moved = pltpu.roll(buckets, shift, 1) if shift else buckets
        for c in range(7):
            at = c * SPAN * CAP + d * CAP
            rows_ref[at : at + CAP, :] = moved[c * CAP : (c + 1) * CAP, :]
    for i in range(CHUNKS):
        message_ref[pl.ds(i, DEVICES, stride=CHUNKS), :] = rows_ref[i * 128 : (i + 1) * 128, :].T


def density_kernel(
    parent_ref, octant_ref, before_ref, own_ref, after_ref, local_ref, maps_ref, out_ref,
    six_ref, picked_ref,
):
    first_parent = 2 * (device_index() - 1)
    for j in range(6):
        source = (before_ref, own_ref, after_ref)[j // 2]
        for c in range(3):
            six_ref[c * 8 + j : c * 8 + j + 1, :] = source[c, j % 2 : j % 2 + 1, :]
    for l in range(LEAVES):
        for c in range(3):
            picked_ref[l : l + 1, c * NEQ : (c + 1) * NEQ] = six_ref[
                pl.ds(c * 8 + parent_ref[l] - first_parent, 1), :
            ]
    lane = iota((1, 2 * LEAVES), 1) % LEAVES
    octants = jnp.zeros((1, 2 * LEAVES), jnp.int32)
    for l in range(LEAVES):
        octants = jnp.where(lane == l, octant_ref[l], octants)
    weights = jnp.concatenate(two(picked_ref[...]), axis=0)
    total = jnp.zeros((3 * NEQ, 2 * LEAVES), F32)
    for o in range(8):
        image = dot(maps_ref[0, o], weights, NT) + dot(maps_ref[1, o], weights, NT)
        total = jnp.where(octants == o, image, total)
    moved = total[:, :LEAVES] + total[:, LEAVES:]
    lane = iota((LEAVES, LANES), 1)
    row = iota((LEAVES, LANES), 0)
    pieces = []
    for c in range(3):
        own = jnp.concatenate([local_ref[c], jnp.zeros((NEQ - LEAVES, NEQ), F32)], axis=0).T
        pieces.append(own[:, :LEAVES] + moved[c * NEQ : (c + 1) * NEQ])
    placed = jnp.zeros((3 * LPTS, LANES), F32)
    for g in range(NEQ // LPTS):
        group = jnp.concatenate([p[g * LPTS : (g + 1) * LPTS] for p in pieces], axis=0)
        place = (lane == row * LPTS + NEAR + g).astype(F32)
        placed = placed + lax.dot_general(
            group, place, NN, precision=HIGHEST, preferred_element_type=F32
        )
    out_ref[...] = placed


def field_kernel(
    arrived_ref, near_ref, density_ref, shell_ref, out_ref,
    turned_ref, tree_ref, source_ref, target_ref, partial_ref, back_ref,
):
    entries = SPAN * CAP
    turned = []
    for i in range(CHUNKS):
        turned.append(arrived_ref[pl.ds(i, DEVICES, stride=CHUNKS), :].T)
    turned = jnp.concatenate(turned, axis=0)
    for c in range(7):
        turned_ref[pl.ds(c, entries, stride=8), :] = turned[c * entries : (c + 1) * entries, :]
    turned_ref[pl.ds(7, entries, stride=8), :] = jnp.zeros((entries, DEVICES), F32)
    tree_ref[SPAN * 32 :, :] = jnp.zeros((1024 - SPAN * 32, 128), F32)
    low_row = iota((128, 128), 0)

    def place(d, carry):
        lows, values = [], []
        for r in range(CAP):
            entry = turned_ref[pl.ds(pl.multiple_of((d * CAP + r) * 8, 8), 8), :]
            slot = entry[6:7, :].astype(jnp.int32) - 1
            lows.append((low_row == (slot & 127)).astype(F32).astype(BF16))
            high = slot >> 7
            parts = three(entry)
            values.append(
                jnp.concatenate(
                    [jnp.where(high == h, part, 0.0) for part in parts for h in range(4)], axis=0
                ).astype(BF16)
            )
        placed = dot(jnp.concatenate(values, axis=1), jnp.concatenate(lows, axis=1), NT)
        tree_ref[pl.ds(pl.multiple_of(d * 32, 32), 32), :] = thirds(placed, 32)
        return carry

    lax.fori_loop(0, SPAN, place, 0, unroll=True)

    terms = [[], [], []]
    for c in range(6):
        turned_c = tree_ref[pl.ds(c, 128, stride=8), :].T
        for s, part in enumerate(three(turned_c)):
            part = part.astype(BF16)
            terms[s].append(
                jnp.concatenate([part[w * LPTS : (w + 1) * LPTS] for w in range(4)], axis=1)
            )
    everything = jnp.concatenate([t for s in range(3) for t in terms[s]], axis=0)
    positions = jnp.concatenate([t for s in range(3) for t in terms[s][:3]], axis=0)
    leaf_row = iota((128, LANES), 0)

    def hot(quarter, row):
        return jnp.concatenate(
            [
                (leaf_row == jnp.where(quarter == w, row, -1)).astype(F32).astype(BF16)
                for w in range(4)
            ],
            axis=0,
        )

    lane = iota((1, LANES), 1)
    spot = lane % LPTS
    near = near_ref[...] - LEAVES * (device_index() - REACH)
    spread = (iota((NEAR, LANES), 0) == spot).astype(F32).astype(BF16)
    own = iota((LEAVES, LANES), 0) == lane // LPTS

    def as_lanes(value):
        value = dot(value.astype(F32).astype(BF16), spread, NN)
        return jnp.sum(jnp.where(own, value, 0.0), axis=0, keepdims=True).astype(jnp.int32)

    near_row = jnp.where(spot < NEAR, as_lanes(near >> 2), -1)
    leaf = lane // LPTS + REACH * LEAVES
    gathered = thirds(dot(everything, hot(as_lanes(near & 3), near_row), NN), 6 * LPTS)
    targets = thirds(dot(positions, hot(leaf & 3, leaf >> 2), NN), 3 * LPTS)
    for k in range(LANES // 128):
        target_ref[k * 96 : (k + 1) * 96, :] = targets[:, k * 128 : (k + 1) * 128]
    axes = [targets[c * LPTS : (c + 1) * LPTS] for c in range(3)]
    centers = [jnp.sum(a, axis=0, keepdims=True) * (1.0 / LPTS) for a in axes]
    half = jnp.maximum(
        jnp.maximum(
            jnp.max(jnp.abs(axes[0] - centers[0]), axis=0, keepdims=True),
            jnp.max(jnp.abs(axes[1] - centers[1]), axis=0, keepdims=True),
        ),
        jnp.max(jnp.abs(axes[2] - centers[2]), axis=0, keepdims=True),
    ) + MARGIN
    far = (spot >= NEAR) & (spot < NEAR + NEQ // LPTS)
    for c in range(3):
        rows = slice(c * LPTS, (c + 1) * LPTS)
        shell = jnp.where(far, centers[c], 0.0) + (SHELL * half) * shell_ref[rows, :]
        source_ref[rows, :] = gathered[rows, :] + shell
    source_ref[3 * LPTS :, :] = gathered[3 * LPTS :, :] + density_ref[...]

    soft = jnp.where(far, 0.0, EPS2)
    for chunk in range(LANES // 128):
        lanes = slice(chunk * 128, (chunk + 1) * 128)
        soft_c = soft[:, lanes]

        def step(p, carry):
            aim = [target_ref[pl.ds(chunk * 96 + c * LPTS + p, 1), :] for c in range(3)]
            sums = None
            for g in range(LPTS // 8):
                at = [source_ref[c * LPTS + g * 8 : c * LPTS + g * 8 + 8, lanes] for c in range(6)]
                gap = [aim[c] - at[c] for c in range(3)]
                square = gap[0] * gap[0] + gap[1] * gap[1] + gap[2] * gap[2] + soft_c
                inverse = lax.rsqrt(square)
                cube = inverse * inverse * inverse
                along = (gap[0] * at[3] + gap[1] * at[4] + gap[2] * at[5]) * cube
                plain = (square + soft_c) * cube
                new = [plain * at[3 + c] + gap[c] * along for c in range(3)]
                sums = new if sums is None else [a + b for a, b in zip(sums, new)]
            for c in range(3):
                partial_ref[pl.ds(chunk * 96 + c * LPTS + p, 1), :] = jnp.sum(
                    sums[c], axis=0, keepdims=True
                )
            return carry

        lax.fori_loop(0, LPTS, step, 0, unroll=8)

    same = (iota((LEAVES, LANES), 1) // LPTS == iota((LEAVES, LANES), 0)).astype(F32)
    partial = jnp.concatenate([partial_ref[k * 96 : (k + 1) * 96, :] for k in range(4)], axis=1)
    by_leaf = [
        lax.dot_general(
            same, partial[c * LPTS : (c + 1) * LPTS, :], NT, precision=HIGHEST,
            preferred_element_type=F32,
        )
        for c in range(3)
    ]
    velocity = jnp.concatenate(by_leaf, axis=0) * (1.0 / EIGHT_PI)
    velocity = jnp.concatenate(three(velocity), axis=0).astype(BF16)
    node_row = iota((LPTS, DEVICES), 0)
    leaf_of = iota((LEAVES, DEVICES), 0)
    back_ref[...] = jnp.zeros_like(back_ref)
    slots, hots = [], []
    for r in range(CAP):
        entry = turned_ref[(REACH * CAP + r) * 8 : (REACH * CAP + r) * 8 + 8, :]
        slot = entry[6:7, :].astype(jnp.int32) - 1
        slots.append(slot)
        hots.append((node_row == (slot & (LPTS - 1))).astype(F32).astype(BF16))
    picked = thirds(dot(velocity, jnp.concatenate(hots, axis=1), NN), 3 * LEAVES)
    for r in range(CAP):
        mine = leaf_of == (slots[r] >> 5)
        for c in range(3):
            piece = picked[c * LEAVES : (c + 1) * LEAVES, r * 128 : (r + 1) * 128]
            back_ref[c * CAP + r : c * CAP + r + 1, :] = jnp.sum(
                jnp.where(mine, piece, 0.0), axis=0, keepdims=True
            )
    out_ref[...] = back_ref[...].T


def split_kernel(blocks_ref, out_ref):
    out_ref[0], out_ref[1] = two(blocks_ref[...])


def fiber_kernel(
    arrived_ref, slot_ref, rank_ref, tension_ref, blocks_ref, out_ref, vector_ref
):
    hot = owner_hot(slot_ref[...]).astype(BF16)
    words = arrived_ref[...].T[: 3 * CAP]
    terms = jnp.concatenate(three(words), axis=0).astype(BF16)
    picked = thirds(dot(terms, hot, NN), 3 * CAP)
    here = iota((CAP, NODES), 0).astype(F32) == rank_ref[...]
    rows = [
        jnp.sum(jnp.where(here, picked[c * CAP : (c + 1) * CAP], 0.0), axis=0, keepdims=True)
        for c in range(3)
    ] + [tension_ref[...]]
    first = iota((1, 128), 1) < 64
    for pair in range(NODES // 128):
        cut = [row[:, pair * 128 : (pair + 1) * 128] for row in rows]
        swapped = [pltpu.roll(row, 64, 1) for row in cut]
        for k in range(2):
            a, b = cut[2 * k], cut[2 * k + 1]
            sa, sb = swapped[2 * k], swapped[2 * k + 1]
            lanes = slice(k * 128, (k + 1) * 128)
            vector_ref[2 * pair : 2 * pair + 1, lanes] = jnp.where(first, a, sb)
            vector_ref[2 * pair + 1 : 2 * pair + 2, lanes] = jnp.where(first, sa, b)
    vector = jnp.concatenate(two(vector_ref[...]), axis=0)
    row = iota((16, 256), 0) % 8
    total = jnp.zeros((16, 256), F32)
    for i in range(8):
        image = dot(vector, blocks_ref[0, i], NT) + dot(vector, blocks_ref[1, i], NT)
        total = jnp.where(row == i, image, total)
    out_ref[...] = total[:8] + total[8:]


def shape(*dims):
    return jax.ShapeDtypeStruct(dims, F32)


def split_up(value, step, mib):
    count, *rest = value.shape
    zeros = (0,) * len(rest)
    return pl.pallas_call(
        split_kernel,
        grid=(count // step,),
        out_shape=jax.ShapeDtypeStruct((2, count, *rest), BF16),
        in_specs=[pl.BlockSpec((step, *rest), lambda i: (i, *zeros))],
        out_specs=pl.BlockSpec((2, step, *rest), lambda i: (0, i, *zeros)),
        cost_estimate=pl.CostEstimate(
            flops=4 * value.size, bytes_accessed=8 * value.size, transcendentals=0
        ),
        compiler_params=grant(mib),
        name="split",
    )(value)


def shifted(value, by):
    pairs = [(i, i + by) for i in range(DEVICES) if 0 <= i + by < DEVICES]
    return lax.ppermute(value, AXES, pairs)


def grant(mib):
    return pltpu.CompilerParams(vmem_limit_bytes=mib << 20)


def exchange(rows):
    return lax.all_to_all(rows.reshape(-1), AXES, 0, 0, tiled=True).reshape(rows.shape)


def local(
    positions, forces, tension, node_slot, leaf_local, parent_local, l2l_maps, leaf_parent,
    leaf_octant, near_list, blocks,
):
    parent_local = parent_local.transpose(1, 0, 2)
    leaf_local = leaf_local.transpose(1, 0, 2)
    slot = node_slot.reshape(1, NODES)
    message, rank = pl.pallas_call(
        pack_kernel,
        out_shape=(shape(CHUNKS * 128, 128), shape(1, NODES)),
        scratch_shapes=[pltpu.VMEM((CHUNKS * 128, DEVICES), F32)],
        cost_estimate=pl.CostEstimate(flops=10**8, bytes_accessed=10**6, transcendentals=0),
        name="pack",
    )(positions, forces, slot)
    message, sent = lax.optimization_barrier((message, parent_local))
    arrived = exchange(message)
    from_before = shifted(sent, 1)
    from_after = shifted(sent, -1)

    vmem = pl.BlockSpec(memory_space=pltpu.VMEM)
    smem = pl.BlockSpec(memory_space=pltpu.SMEM)
    density = pl.pallas_call(
        density_kernel,
        out_shape=shape(3 * LPTS, LANES),
        in_specs=[smem, smem, vmem, vmem, vmem, vmem, vmem],
        scratch_shapes=[
            pltpu.VMEM((24, NEQ), F32),
            pltpu.VMEM((LEAVES, 3 * NEQ), F32),
        ],
        cost_estimate=pl.CostEstimate(flops=10**9, bytes_accessed=5 * 10**6, transcendentals=0),
        compiler_params=grant(16),
        name="density",
    )(
        leaf_parent, leaf_octant, from_before, parent_local, from_after,
        leaf_local, split_up(l2l_maps, 2, MAPS_GRANT),
    )
    back = pl.pallas_call(
        field_kernel,
        out_shape=shape(DEVICES, 128),
        scratch_shapes=[
            pltpu.VMEM((SPAN * CAP * 8, DEVICES), F32),
            pltpu.VMEM((1024, 128), F32),
            pltpu.VMEM((6 * LPTS, LANES), F32),
            pltpu.VMEM((12 * LPTS, 128), F32),
            pltpu.VMEM((12 * LPTS, 128), F32),
            pltpu.VMEM((128, DEVICES), F32),
        ],
        cost_estimate=pl.CostEstimate(flops=10**9, bytes_accessed=2 * 10**6, transcendentals=0),
        compiler_params=grant(16),
        name="field",
    )(arrived, near_list, density, jnp.asarray(shell_table()))
    returned = exchange(back)
    return pl.pallas_call(
        fiber_kernel,
        out_shape=shape(8, 256),
        scratch_shapes=[pltpu.VMEM((8, 256), F32)],
        cost_estimate=pl.CostEstimate(flops=10**8, bytes_accessed=2 * 10**6, transcendentals=0),
        compiler_params=grant(8),
        name="fiber",
    )(returned, slot, rank, tension.reshape(1, NODES), split_up(blocks, 2, 4))


def solution(mesh):
    both = ("aa", "ba")
    in_specs = (
        P(None, both), P(None, both), P(both), P(both), P(both, None, None), P(both, None, None),
        P(), P(both), P(both), P(both, None), P(both, None, None),
    )
    return jax.shard_map(
        local, mesh=mesh, in_specs=in_specs, out_specs=P(both, None), check_vma=False
    )
```

```python
import jax
import jax.numpy as jnp
import numpy as np
from jax import lax
from jax.experimental import pallas as pl
from jax.experimental.pallas import tpu as pltpu
from jax.sharding import PartitionSpec as P

DEVICES = 128
NODES = 512
CAP = 16
REACH = 8
SPAN = 2 * REACH + 1
LEAVES = 16
LPTS = 32
NEAR = 27
NEQ = 128
LANES = LEAVES * LPTS
GROUPS = NEQ // LPTS
FAR = GROUPS * LEAVES
WORDS = 7 * SPAN * CAP
CHUNKS = 15
EPS2 = 0.05**2
MARGIN = 0.05
SHELL = 2.95
GOLDEN = 2.399963229728653
EIGHT_PI = 25.132741228718345
AXES = ("aa", "ba")
HIGHEST = lax.Precision.HIGHEST
F32, BF16 = jnp.float32, jnp.bfloat16
NT = (((1,), (1,)), ((), ()))
NN = (((1,), (0,)), ((), ()))


def iota(shape, dim):
    return lax.broadcasted_iota(jnp.int32, shape, dim)


def three(x):
    high = x.astype(BF16).astype(F32)
    rest = x - high
    middle = rest.astype(BF16).astype(F32)
    return high, middle, rest - middle


def two(x):
    high = x.astype(BF16)
    return high, (x - high.astype(F32)).astype(BF16)


def dot(a, b, dims):
    return lax.dot_general(a, b, dims, preferred_element_type=F32)


def thirds(x, rows):
    return x[:rows] + x[rows : 2 * rows] + x[2 * rows :]


def shell_table():
    q = np.arange(NEQ, dtype=np.float32) + np.float32(0.5)
    h = (np.float32(1.0) - np.float32(2.0) * q / np.float32(NEQ)).astype(np.float32)
    radius = np.sqrt(np.maximum(np.float32(1.0) - h * h, 0)).astype(np.float32)
    angle = (q * np.float32(GOLDEN)).astype(np.float32)
    w = np.stack([radius * np.cos(angle), radius * np.sin(angle), h]).astype(np.float32)
    s = w / np.max(np.abs(w), axis=0, keepdims=True)
    table = np.zeros((3, LPTS, 128), np.float32)
    for g in range(GROUPS):
        table[:, :, g * LEAVES : (g + 1) * LEAVES] = s[:, g * LPTS : (g + 1) * LPTS, None]
    return table.reshape(3 * LPTS, 128)


def lane_place():
    lane = iota((1, LANES), 1)
    near = lane - FAR
    leaf = ((near.astype(F32) + 0.5) * (1.0 / NEAR)).astype(jnp.int32)
    place = near - leaf * NEAR
    is_near = (lane >= FAR) & (lane < FAR + LEAVES * NEAR)
    leaf = jnp.where(lane < FAR, lane & (LEAVES - 1), jnp.where(is_near, leaf, 0))
    return leaf, jnp.where(is_near, place, -1)


def device_index():
    return lax.axis_index("aa") * 16 + lax.axis_index("ba")


def owner_hot(slot):
    return (iota((DEVICES, NODES), 0) == (slot >> 9)).astype(F32)


def pack_kernel(pos_ref, force_ref, slot_ref, message_ref, rank_ref, rows_ref):
    slot = slot_ref[...]
    hot = owner_hot(slot)
    hot_b = hot.astype(BF16)
    before = (iota((NODES, NODES), 0) < iota((NODES, NODES), 1)).astype(F32).astype(BF16)
    rank = jnp.sum(hot * dot(hot_b, before, NN), axis=0, keepdims=True)
    rank_ref[...] = rank
    here = iota((CAP, NODES), 0).astype(F32) == rank
    within = (slot & (NODES - 1)).astype(F32) + 1.0
    payload = [pos_ref[c : c + 1, :] for c in range(3)]
    payload += [force_ref[c : c + 1, :] for c in range(3)] + [within]
    spread = jnp.concatenate([jnp.where(here, row, 0.0) for row in payload], axis=0)
    terms = jnp.concatenate(three(spread), axis=0).astype(BF16)
    buckets = thirds(dot(terms, hot_b, NT), 7 * CAP)
    rows_ref[WORDS:, :] = jnp.zeros((CHUNKS * 128 - WORDS, DEVICES), F32)
    for d in range(SPAN):
        shift = (REACH - d) % DEVICES
        moved = pltpu.roll(buckets, shift, 1) if shift else buckets
        for c in range(7):
            at = c * SPAN * CAP + d * CAP
            rows_ref[at : at + CAP, :] = moved[c * CAP : (c + 1) * CAP, :]
    for i in range(CHUNKS):
        message_ref[pl.ds(i, DEVICES, stride=CHUNKS), :] = rows_ref[i * 128 : (i + 1) * 128, :].T


def prepare_kernel(near_ref, maps_ref, split_ref, near_hot_ref, own_hot_ref, rows_ref):
    step = pl.program_id(0)

    @pl.when(step == 0)
    def _():
        leaf, place = lane_place()
        near = near_ref[...] - LEAVES * (device_index() - REACH)
        spread = (iota((NEAR, LANES), 0) == place).astype(F32).astype(BF16)
        own = iota((LEAVES, LANES), 0) == leaf
        values = jnp.concatenate([near & 3, near >> 2], axis=0).astype(F32).astype(BF16)
        values = dot(values, spread, NN)
        for k in range(2):
            value = jnp.where(own, values[k * LEAVES : (k + 1) * LEAVES], 0.0)
            value = jnp.sum(value, axis=0, keepdims=True).astype(jnp.int32)
            rows_ref[k : k + 1, :] = jnp.where(place >= 0, value, -1)
        rows_ref[2:3, :] = leaf & 3
        rows_ref[3:4, :] = (leaf + REACH * LEAVES) >> 2

    split_ref[0], split_ref[1] = two(maps_ref[...])
    leaf_row = iota((128, LANES), 0)
    for k, ref in enumerate((near_hot_ref, own_hot_ref)):
        row = jnp.where(rows_ref[2 * k : 2 * k + 1, :] == step, rows_ref[2 * k + 1 : 2 * k + 2, :], -1)
        ref[...] = (leaf_row == row).astype(F32).astype(BF16)


def density_kernel(
    parent_ref, octant_ref, before_ref, own_ref, after_ref, local_ref, maps_ref, out_ref,
    six_ref, picked_ref,
):
    first_parent = 2 * (device_index() - 1)
    for j in range(6):
        source = (before_ref, own_ref, after_ref)[j // 2]
        for c in range(3):
            six_ref[c * 8 + j : c * 8 + j + 1, :] = source[c, j % 2 : j % 2 + 1, :]
    lane = iota((1, 128), 1) % LEAVES
    octants = jnp.zeros((1, 128), jnp.int32)
    for l in range(LEAVES):
        octants = jnp.where(lane == l, octant_ref[l], octants)
        for c in range(3):
            picked_ref[l : l + 1, c * NEQ : (c + 1) * NEQ] = six_ref[
                pl.ds(c * 8 + parent_ref[l] - first_parent, 1), :
            ]
    high, low = two(picked_ref[...])
    weights = jnp.concatenate([high] * GROUPS + [low] * GROUPS, axis=0)
    total = jnp.zeros((3 * NEQ, 128), F32)
    for o in range(8):
        image = dot(maps_ref[0, o], weights, NT) + dot(maps_ref[1, o], weights, NT)
        total = jnp.where(octants == o, image, total)
    group = iota((1, 128), 1) // LEAVES
    nothing = jnp.zeros((NEQ - FAR, NEQ), F32)
    for c in range(3):
        local = jnp.concatenate([local_ref[c]] * GROUPS + [nothing], axis=0).T
        moved = total[c * NEQ : (c + 1) * NEQ]
        placed = jnp.zeros((LPTS, 128), F32)
        for g in range(GROUPS):
            rows = slice(g * LPTS, (g + 1) * LPTS)
            here = group % GROUPS == g
            placed = jnp.where(here, moved[rows] + local[rows], placed)
        placed = placed + pltpu.roll(placed, 128 - FAR, 1)
        out_ref[c * LPTS : (c + 1) * LPTS, :] = jnp.where(group < GROUPS, placed, 0.0)


def field_kernel(
    arrived_ref, near_hot_ref, own_hot_ref, density_ref, shell_ref, out_ref,
    turned_ref, tree_ref, source_ref, target_ref, partial_ref, back_ref,
):
    entries = SPAN * CAP
    turned = []
    for i in range(CHUNKS):
        turned.append(arrived_ref[pl.ds(i, DEVICES, stride=CHUNKS), :].T)
    turned = jnp.concatenate(turned, axis=0)
    for c in range(7):
        turned_ref[pl.ds(c, entries, stride=8), :] = turned[c * entries : (c + 1) * entries, :]
    turned_ref[pl.ds(7, entries, stride=8), :] = jnp.zeros((entries, DEVICES), F32)
    tree_ref[SPAN * 32 :, :] = jnp.zeros((1024 - SPAN * 32, 128), F32)
    low_row = iota((128, 128), 0)

    def place(d, carry):
        lows, values = [], []
        for r in range(CAP):
            entry = turned_ref[pl.ds(pl.multiple_of((d * CAP + r) * 8, 8), 8), :]
            slot = entry[6:7, :].astype(jnp.int32) - 1
            lows.append((low_row == (slot & 127)).astype(F32).astype(BF16))
            high = slot >> 7
            parts = three(entry)
            values.append(
                jnp.concatenate(
                    [jnp.where(high == h, part, 0.0) for part in parts for h in range(4)], axis=0
                ).astype(BF16)
            )
        placed = dot(jnp.concatenate(values, axis=1), jnp.concatenate(lows, axis=1), NT)
        tree_ref[pl.ds(pl.multiple_of(d * 32, 32), 32), :] = thirds(placed, 32)
        return carry

    lax.fori_loop(0, SPAN, place, 0, unroll=True)

    terms = [[], [], []]
    for c in range(6):
        turned_c = tree_ref[pl.ds(c, 128, stride=8), :].T
        for s, part in enumerate(three(turned_c)):
            part = part.astype(BF16)
            terms[s].append(
                jnp.concatenate([part[w * LPTS : (w + 1) * LPTS] for w in range(4)], axis=1)
            )
    everything = jnp.concatenate([t for s in range(3) for t in terms[s]], axis=0)
    positions = jnp.concatenate([t for s in range(3) for t in terms[s][:3]], axis=0)
    gathered = thirds(dot(everything, near_hot_ref[...], NN), 6 * LPTS)
    targets = thirds(dot(positions, own_hot_ref[...], NN), 3 * LPTS)
    for k in range(LANES // 128):
        target_ref[k * 96 : (k + 1) * 96, :] = targets[:, k * 128 : (k + 1) * 128]
    axes = [targets[c * LPTS : (c + 1) * LPTS] for c in range(3)]
    centers = [jnp.sum(a, axis=0, keepdims=True) * (1.0 / LPTS) for a in axes]
    half = jnp.maximum(
        jnp.maximum(
            jnp.max(jnp.abs(axes[0] - centers[0]), axis=0, keepdims=True),
            jnp.max(jnp.abs(axes[1] - centers[1]), axis=0, keepdims=True),
        ),
        jnp.max(jnp.abs(axes[2] - centers[2]), axis=0, keepdims=True),
    ) + MARGIN
    for c in range(3):
        rows = slice(c * LPTS, (c + 1) * LPTS)
        more = slice((3 + c) * LPTS, (4 + c) * LPTS)
        first = gathered[rows, :128] + (SHELL * half[:, :128]) * shell_ref[rows, :]
        source_ref[rows, :128] = first + jnp.where(iota((1, 128), 1) < FAR, centers[c][:, :128], 0.0)
        source_ref[rows, 128:] = gathered[rows, 128:]
        source_ref[more, :128] = gathered[more, :128] + density_ref[rows, :]
        source_ref[more, 128:] = gathered[more, 128:]
    soft = jnp.where(iota((1, LANES), 1) < FAR, 0.0, EPS2)
    for chunk in range(LANES // 128):
        lanes = slice(chunk * 128, (chunk + 1) * 128)
        soft_c = soft[:, lanes]

        def step(p, carry):
            aim = [target_ref[pl.ds(chunk * 96 + c * LPTS + p, 1), :] for c in range(3)]
            sums = None
            for g in range(LPTS // 8):
                at = [source_ref[c * LPTS + g * 8 : c * LPTS + g * 8 + 8, lanes] for c in range(6)]
                gap = [aim[c] - at[c] for c in range(3)]
                square = gap[0] * gap[0] + gap[1] * gap[1] + gap[2] * gap[2] + soft_c
                inverse = lax.rsqrt(square)
                cube = inverse * inverse * inverse
                along = (gap[0] * at[3] + gap[1] * at[4] + gap[2] * at[5]) * cube
                plain = (square + soft_c) * cube
                new = [plain * at[3 + c] + gap[c] * along for c in range(3)]
                sums = new if sums is None else [a + b for a, b in zip(sums, new)]
            for c in range(3):
                partial_ref[pl.ds(chunk * 96 + c * LPTS + p, 1), :] = jnp.sum(
                    sums[c], axis=0, keepdims=True
                )
            return carry

        lax.fori_loop(0, LPTS, step, 0, unroll=8)

    same = (iota((LEAVES, LANES), 0) == lane_place()[0]).astype(F32).astype(BF16)
    same = jnp.concatenate([same] * 3, axis=1)
    partial = jnp.concatenate([partial_ref[k * 96 : (k + 1) * 96, :] for k in range(4)], axis=1)
    partial = jnp.concatenate(three(partial), axis=1).astype(BF16)
    by_leaf = [dot(same, partial[c * LPTS : (c + 1) * LPTS, :], NT) for c in range(3)]
    velocity = jnp.concatenate(by_leaf, axis=0) * (1.0 / EIGHT_PI)
    velocity = jnp.concatenate(three(velocity), axis=0).astype(BF16)
    node_row = iota((LPTS, DEVICES), 0)
    leaf_of = iota((LEAVES, DEVICES), 0)
    back_ref[...] = jnp.zeros_like(back_ref)
    slots, hots = [], []
    for r in range(CAP):
        entry = turned_ref[(REACH * CAP + r) * 8 : (REACH * CAP + r) * 8 + 8, :]
        slot = entry[6:7, :].astype(jnp.int32) - 1
        slots.append(slot)
        hots.append((node_row == (slot & (LPTS - 1))).astype(F32).astype(BF16))
    picked = thirds(dot(velocity, jnp.concatenate(hots, axis=1), NN), 3 * LEAVES)
    for r in range(CAP):
        mine = leaf_of == (slots[r] >> 5)
        for c in range(3):
            piece = picked[c * LEAVES : (c + 1) * LEAVES, r * 128 : (r + 1) * 128]
            back_ref[c * CAP + r : c * CAP + r + 1, :] = jnp.sum(
                jnp.where(mine, piece, 0.0), axis=0, keepdims=True
            )
    out_ref[...] = back_ref[...].T


def split_kernel(blocks_ref, out_ref):
    for i in range(2):
        out_ref[0, i], out_ref[1, i] = two(blocks_ref[i].T)


def fiber_kernel(
    arrived_ref, slot_ref, rank_ref, tension_ref, blocks_ref, out_ref, vector_ref
):
    hot = owner_hot(slot_ref[...]).astype(BF16)
    words = arrived_ref[...].T[: 3 * CAP]
    terms = jnp.concatenate(three(words), axis=0).astype(BF16)
    picked = thirds(dot(terms, hot, NN), 3 * CAP)
    here = iota((CAP, NODES), 0).astype(F32) == rank_ref[...]
    rows = [
        jnp.sum(jnp.where(here, picked[c * CAP : (c + 1) * CAP], 0.0), axis=0, keepdims=True)
        for c in range(3)
    ] + [tension_ref[...]]
    first = iota((1, 128), 1) < 64
    for pair in range(NODES // 128):
        cut = [row[:, pair * 128 : (pair + 1) * 128] for row in rows]
        swapped = [pltpu.roll(row, 64, 1) for row in cut]
        for k in range(2):
            a, b = cut[2 * k], cut[2 * k + 1]
            sa, sb = swapped[2 * k], swapped[2 * k + 1]
            lanes = slice(k * 128, (k + 1) * 128)
            vector_ref[2 * pair : 2 * pair + 1, lanes] = jnp.where(first, a, sb)
            vector_ref[2 * pair + 1 : 2 * pair + 2, lanes] = jnp.where(first, sa, b)
    vector = jnp.concatenate(two(vector_ref[...]), axis=0)
    row = iota((16, 256), 0) % 8
    total = jnp.zeros((16, 256), F32)
    for i in range(8):
        image = dot(vector, blocks_ref[0, i], NN) + dot(vector, blocks_ref[1, i], NN)
        total = jnp.where(row == i, image, total)
    out_ref[...] = total[:8] + total[8:]


def shape(*dims):
    return jax.ShapeDtypeStruct(dims, F32)


def shifted(value, by):
    pairs = [(i, i + by) for i in range(DEVICES) if 0 <= i + by < DEVICES]
    return lax.ppermute(value, AXES, pairs)


def grant(mib):
    return pltpu.CompilerParams(vmem_limit_bytes=mib << 20)


def exchange(rows):
    return lax.all_to_all(rows.reshape(-1), AXES, 0, 0, tiled=True).reshape(rows.shape)


def local(
    positions, forces, tension, node_slot, leaf_local, parent_local, l2l_maps, leaf_parent,
    leaf_octant, near_list, blocks,
):
    parent_local = parent_local.transpose(1, 0, 2)
    leaf_local = leaf_local.transpose(1, 0, 2)
    slot = node_slot.reshape(1, NODES)
    message, rank = pl.pallas_call(
        pack_kernel,
        out_shape=(shape(CHUNKS * 128, 128), shape(1, NODES)),
        scratch_shapes=[pltpu.VMEM((CHUNKS * 128, DEVICES), F32)],
        cost_estimate=pl.CostEstimate(flops=10**8, bytes_accessed=10**6, transcendentals=0),
        name="pack",
    )(positions, forces, slot)
    message, sent = lax.optimization_barrier((message, parent_local))
    arrived = exchange(message)
    from_before = shifted(sent, 1)
    from_after = shifted(sent, -1)

    vmem = pl.BlockSpec(memory_space=pltpu.VMEM)
    smem = pl.BlockSpec(memory_space=pltpu.SMEM)
    maps, near_hot, own_hot = pl.pallas_call(
        prepare_kernel,
        grid=(4,),
        out_shape=(
            jax.ShapeDtypeStruct((2, 8, 384, 384), BF16),
            jax.ShapeDtypeStruct((LANES, LANES), BF16),
            jax.ShapeDtypeStruct((LANES, LANES), BF16),
        ),
        in_specs=[
            pl.BlockSpec((LEAVES, NEAR), lambda i: (0, 0)),
            pl.BlockSpec((2, 384, 384), lambda i: (i, 0, 0)),
        ],
        out_specs=(
            pl.BlockSpec((2, 2, 384, 384), lambda i: (0, i, 0, 0)),
            pl.BlockSpec((128, LANES), lambda i: (i, 0)),
            pl.BlockSpec((128, LANES), lambda i: (i, 0)),
        ),
        scratch_shapes=[pltpu.VMEM((8, LANES), jnp.int32)],
        cost_estimate=pl.CostEstimate(flops=5 * 10**6, bytes_accessed=10**7, transcendentals=0),
        compiler_params=grant(8),
        name="prepare",
    )(near_list, l2l_maps)
    split = pl.pallas_call(
        split_kernel,
        grid=(4,),
        out_shape=jax.ShapeDtypeStruct((2, 8, 256, 256), BF16),
        in_specs=[pl.BlockSpec((2, 256, 256), lambda i: (i, 0, 0))],
        out_specs=pl.BlockSpec((2, 2, 256, 256), lambda i: (0, i, 0, 0)),
        cost_estimate=pl.CostEstimate(flops=2 * 10**6, bytes_accessed=4 * 10**6, transcendentals=0),
        compiler_params=grant(4),
        name="split",
    )(blocks)
    density = pl.pallas_call(
        density_kernel,
        out_shape=shape(3 * LPTS, 128),
        in_specs=[smem, smem, vmem, vmem, vmem, vmem, vmem],
        scratch_shapes=[
            pltpu.VMEM((24, NEQ), F32),
            pltpu.VMEM((LEAVES, 3 * NEQ), F32),
        ],
        cost_estimate=pl.CostEstimate(flops=10**9, bytes_accessed=5 * 10**6, transcendentals=0),
        compiler_params=grant(16),
        name="density",
    )(
        leaf_parent, leaf_octant, from_before, parent_local, from_after,
        leaf_local, maps,
    )
    back = pl.pallas_call(
        field_kernel,
        out_shape=shape(DEVICES, 128),
        scratch_shapes=[
            pltpu.VMEM((SPAN * CAP * 8, DEVICES), F32),
            pltpu.VMEM((1024, 128), F32),
            pltpu.VMEM((6 * LPTS, LANES), F32),
            pltpu.VMEM((12 * LPTS, 128), F32),
            pltpu.VMEM((12 * LPTS, 128), F32),
            pltpu.VMEM((128, DEVICES), F32),
        ],
        cost_estimate=pl.CostEstimate(flops=10**9, bytes_accessed=2 * 10**6, transcendentals=0),
        compiler_params=grant(16),
        name="field",
    )(arrived, near_hot, own_hot, density, jnp.asarray(shell_table()))
    returned = exchange(back)
    return pl.pallas_call(
        fiber_kernel,
        out_shape=shape(8, 256),
        scratch_shapes=[pltpu.VMEM((8, 256), F32)],
        cost_estimate=pl.CostEstimate(flops=10**8, bytes_accessed=2 * 10**6, transcendentals=0),
        compiler_params=grant(8),
        name="fiber",
    )(returned, slot, rank, tension.reshape(1, NODES), split)


def solution(mesh):
    both = ("aa", "ba")
    in_specs = (
        P(None, both), P(None, both), P(both), P(both), P(both, None, None), P(both, None, None),
        P(), P(both), P(both), P(both, None), P(both, None, None),
    )
    return jax.shard_map(
        local, mesh=mesh, in_specs=in_specs, out_specs=P(both, None), check_vma=False
    )
```

```python
import jax
import jax.numpy as jnp
import numpy as np
from jax import lax
from jax.experimental import pallas as pl
from jax.experimental.pallas import tpu as pltpu
from jax.sharding import PartitionSpec as P

DEVICES = 128
NODES = 512
CAP = 16
REACH = 8
SPAN = 2 * REACH + 1
LEAVES = 16
LPTS = 32
NEAR = 27
NEQ = 128
LANES = LEAVES * LPTS
GROUPS = NEQ // LPTS
FAR = GROUPS * LEAVES
WORDS = 7 * SPAN * CAP
CHUNKS = 15
EPS2 = 0.05**2
MARGIN = 0.05
SHELL = 2.95
GOLDEN = 2.399963229728653
EIGHT_PI = 25.132741228718345
AXES = ("aa", "ba")
HIGHEST = lax.Precision.HIGHEST
F32, BF16 = jnp.float32, jnp.bfloat16
NT = (((1,), (1,)), ((), ()))
NN = (((1,), (0,)), ((), ()))


def iota(shape, dim):
    return lax.broadcasted_iota(jnp.int32, shape, dim)


def three(x):
    high = x.astype(BF16).astype(F32)
    rest = x - high
    middle = rest.astype(BF16).astype(F32)
    return high, middle, rest - middle


def two(x):
    high = x.astype(BF16)
    return high, (x - high.astype(F32)).astype(BF16)


def dot(a, b, dims):
    return lax.dot_general(a, b, dims, preferred_element_type=F32)


def thirds(x, rows):
    return x[:rows] + x[rows : 2 * rows] + x[2 * rows :]


def shell_table():
    q = np.arange(NEQ, dtype=np.float32) + np.float32(0.5)
    h = (np.float32(1.0) - np.float32(2.0) * q / np.float32(NEQ)).astype(np.float32)
    radius = np.sqrt(np.maximum(np.float32(1.0) - h * h, 0)).astype(np.float32)
    angle = (q * np.float32(GOLDEN)).astype(np.float32)
    w = np.stack([radius * np.cos(angle), radius * np.sin(angle), h]).astype(np.float32)
    s = w / np.max(np.abs(w), axis=0, keepdims=True)
    table = np.zeros((3, LPTS, 128), np.float32)
    for g in range(GROUPS):
        table[:, :, g * LEAVES : (g + 1) * LEAVES] = s[:, g * LPTS : (g + 1) * LPTS, None]
    return table.reshape(3 * LPTS, 128)


def lane_place():
    lane = iota((1, LANES), 1)
    near = lane - FAR
    leaf = ((near.astype(F32) + 0.5) * (1.0 / NEAR)).astype(jnp.int32)
    place = near - leaf * NEAR
    is_near = (lane >= FAR) & (lane < FAR + LEAVES * NEAR)
    leaf = jnp.where(lane < FAR, lane & (LEAVES - 1), jnp.where(is_near, leaf, 0))
    return leaf, jnp.where(is_near, place, -1)


def device_index():
    return lax.axis_index("aa") * 16 + lax.axis_index("ba")


def owner_hot(slot):
    return (iota((DEVICES, NODES), 0) == (slot >> 9)).astype(F32)


def pack_kernel(pos_ref, force_ref, slot_ref, message_ref, rank_ref, rows_ref):
    slot = slot_ref[...]
    hot = owner_hot(slot)
    hot_b = hot.astype(BF16)
    before = (iota((NODES, NODES), 0) < iota((NODES, NODES), 1)).astype(F32).astype(BF16)
    rank = jnp.sum(hot * dot(hot_b, before, NN), axis=0, keepdims=True)
    rank_ref[...] = rank
    here = iota((CAP, NODES), 0).astype(F32) == rank
    within = (slot & (NODES - 1)).astype(F32) + 1.0
    payload = [pos_ref[c : c + 1, :] for c in range(3)]
    payload += [force_ref[c : c + 1, :] for c in range(3)] + [within]
    spread = jnp.concatenate([jnp.where(here, row, 0.0) for row in payload], axis=0)
    terms = jnp.concatenate(three(spread), axis=0).astype(BF16)
    buckets = thirds(dot(terms, hot_b, NT), 7 * CAP)
    rows_ref[WORDS:, :] = jnp.zeros((CHUNKS * 128 - WORDS, DEVICES), F32)
    for d in range(SPAN):
        shift = (REACH - d) % DEVICES
        moved = pltpu.roll(buckets, shift, 1) if shift else buckets
        rows_ref[d * 7 * CAP : (d + 1) * 7 * CAP, :] = moved
    for i in range(CHUNKS):
        message_ref[pl.ds(i, DEVICES, stride=CHUNKS), :] = rows_ref[i * 128 : (i + 1) * 128, :].T


def prepare_kernel(near_ref, maps_ref, split_ref, near_hot_ref, own_hot_ref, rows_ref):
    step = pl.program_id(0)

    @pl.when(step == 0)
    def _():
        leaf, place = lane_place()
        near = near_ref[...] - LEAVES * (device_index() - REACH)
        spread = (iota((NEAR, LANES), 0) == place).astype(F32).astype(BF16)
        own = iota((LEAVES, LANES), 0) == leaf
        values = jnp.concatenate([near & 3, near >> 2], axis=0).astype(F32).astype(BF16)
        values = dot(values, spread, NN)
        for k in range(2):
            value = jnp.where(own, values[k * LEAVES : (k + 1) * LEAVES], 0.0)
            value = jnp.sum(value, axis=0, keepdims=True).astype(jnp.int32)
            rows_ref[k : k + 1, :] = jnp.where(place >= 0, value, -1)
        rows_ref[2:3, :] = leaf & 3
        rows_ref[3:4, :] = (leaf + REACH * LEAVES) >> 2

    split_ref[:, :, : 3 * NEQ], split_ref[:, :, 3 * NEQ :] = two(maps_ref[...])
    leaf_row = iota((128, LANES), 0)
    for k, ref in enumerate((near_hot_ref, own_hot_ref)):
        row = jnp.where(rows_ref[2 * k : 2 * k + 1, :] == step, rows_ref[2 * k + 1 : 2 * k + 2, :], -1)
        ref[...] = (leaf_row == row).astype(F32).astype(BF16)


def density_kernel(
    parent_ref, octant_ref, before_ref, own_ref, after_ref, local_ref, maps_ref, out_ref,
    six_ref, picked_ref,
):
    first_parent = 2 * (device_index() - 1)
    for j in range(6):
        source = (before_ref, own_ref, after_ref)[j // 2]
        for c in range(3):
            six_ref[c * 8 + j : c * 8 + j + 1, :] = source[c, j % 2 : j % 2 + 1, :]
    lane = iota((1, 128), 1) % LEAVES
    octants = jnp.zeros((1, 128), jnp.int32)
    for l in range(LEAVES):
        octants = jnp.where(lane == l, octant_ref[l], octants)
        for c in range(3):
            picked_ref[l : l + 1, c * NEQ : (c + 1) * NEQ] = six_ref[
                pl.ds(c * 8 + parent_ref[l] - first_parent, 1), :
            ]
    high, low = two(picked_ref[...])
    weights = jnp.concatenate([high] * GROUPS + [low] * GROUPS, axis=0)
    weights = jnp.concatenate([weights, weights], axis=1)
    total = jnp.zeros((3 * NEQ, 128), F32)
    for o in range(8):
        image = dot(maps_ref[o], weights, NT)
        total = jnp.where(octants == o, image, total)
    group = iota((1, 128), 1) // LEAVES
    nothing = jnp.zeros((NEQ - FAR, NEQ), F32)
    for c in range(3):
        local = jnp.concatenate([local_ref[c]] * GROUPS + [nothing], axis=0).T
        moved = total[c * NEQ : (c + 1) * NEQ]
        placed = jnp.zeros((LPTS, 128), F32)
        for g in range(GROUPS):
            rows = slice(g * LPTS, (g + 1) * LPTS)
            here = group % GROUPS == g
            placed = jnp.where(here, moved[rows] + local[rows], placed)
        placed = placed + pltpu.roll(placed, 128 - FAR, 1)
        out_ref[c * LPTS : (c + 1) * LPTS, :] = jnp.where(group < GROUPS, placed, 0.0)


def field_kernel(
    arrived_ref, near_hot_ref, own_hot_ref, density_ref, shell_ref, out_ref,
    turned_ref, tree_ref, source_ref, target_ref, partial_ref, back_ref,
):
    turned = [arrived_ref[pl.ds(i, DEVICES, stride=CHUNKS), :].T for i in range(CHUNKS)]
    tree_ref[SPAN * 32 :, :] = jnp.zeros((1024 - SPAN * 32, 128), F32)
    low_row = iota((128, 128), 0).astype(F32).astype(BF16)
    half_row = [(iota((16, 128), 0) // 8 + k).astype(F32).astype(BF16) for k in (0, 2)]
    one, zero = jnp.ones((16, 128), BF16), jnp.zeros((16, 128), BF16)

    def narrow(row):
        return jnp.broadcast_to(row.astype(F32), (16, 128)).astype(BF16)

    def place(d):
        lows, values = [], []
        for r in range(CAP):
            entry = turned_ref[(d * CAP + r) * 8 : (d * CAP + r) * 8 + 8, :]
            slot = entry[6:7, :].astype(jnp.int32) - 1
            low, high = narrow(slot & 127), narrow(slot >> 7)
            lows.append(
                jnp.concatenate(
                    [jnp.where(low_row[k : k + 16] == low, one, zero) for k in range(0, 128, 16)],
                    axis=0,
                )
            )
            here = [row == high for row in half_row]
            parts = [jnp.concatenate([part, part], axis=0).astype(BF16) for part in three(entry)]
            values.append(
                jnp.concatenate([jnp.where(h, part, zero) for part in parts for h in here], axis=0)
            )
        placed = dot(jnp.concatenate(lows, axis=1), jnp.concatenate(values, axis=1), NT).T
        tree_ref[d * 32 : (d + 1) * 32, :] = thirds(placed, 32)

    for d in range(SPAN):
        for c in range(7):
            at = d * 7 * CAP + c * CAP
            turned_ref[pl.ds(d * 8 * CAP + c, CAP, stride=8), :] = turned[at // 128][
                at % 128 : at % 128 + CAP, :
            ]
        turned_ref[pl.ds(d * 8 * CAP + 7, CAP, stride=8), :] = jnp.zeros((CAP, DEVICES), F32)
        place(d)

    terms = [[], [], []]
    for c in range(6):
        turned_c = tree_ref[pl.ds(c, 128, stride=8), :].T
        for s, part in enumerate(three(turned_c)):
            part = part.astype(BF16)
            terms[s].append(
                jnp.concatenate([part[w * LPTS : (w + 1) * LPTS] for w in range(4)], axis=1)
            )
    everything = jnp.concatenate([t for s in range(3) for t in terms[s]], axis=0)
    positions = jnp.concatenate([t for s in range(3) for t in terms[s][:3]], axis=0)
    gathered = thirds(dot(everything, near_hot_ref[...], NN), 6 * LPTS)
    targets = thirds(dot(positions, own_hot_ref[...], NN), 3 * LPTS)
    for k in range(LANES // 128):
        target_ref[k * 96 : (k + 1) * 96, :] = targets[:, k * 128 : (k + 1) * 128]
    axes = [targets[c * LPTS : (c + 1) * LPTS] for c in range(3)]
    centers = [jnp.sum(a, axis=0, keepdims=True) * (1.0 / LPTS) for a in axes]
    half = jnp.maximum(
        jnp.maximum(
            jnp.max(jnp.abs(axes[0] - centers[0]), axis=0, keepdims=True),
            jnp.max(jnp.abs(axes[1] - centers[1]), axis=0, keepdims=True),
        ),
        jnp.max(jnp.abs(axes[2] - centers[2]), axis=0, keepdims=True),
    ) + MARGIN
    for c in range(3):
        rows = slice(c * LPTS, (c + 1) * LPTS)
        more = slice((3 + c) * LPTS, (4 + c) * LPTS)
        first = gathered[rows, :128] + (SHELL * half[:, :128]) * shell_ref[rows, :]
        source_ref[rows, :128] = first + jnp.where(iota((1, 128), 1) < FAR, centers[c][:, :128], 0.0)
        source_ref[rows, 128:] = gathered[rows, 128:]
        source_ref[more, :128] = gathered[more, :128] + density_ref[rows, :]
        source_ref[more, 128:] = gathered[more, 128:]
    soft = jnp.where(iota((1, LANES), 1) < FAR, 0.0, EPS2)
    for chunk in range(LANES // 128):
        lanes = slice(chunk * 128, (chunk + 1) * 128)
        soft_c = soft[:, lanes]

        def step(p, carry):
            aim = [target_ref[pl.ds(chunk * 96 + c * LPTS + p, 1), :] for c in range(3)]
            sums = None
            for g in range(LPTS // 8):
                at = [source_ref[c * LPTS + g * 8 : c * LPTS + g * 8 + 8, lanes] for c in range(6)]
                gap = [aim[c] - at[c] for c in range(3)]
                square = gap[0] * gap[0] + gap[1] * gap[1] + gap[2] * gap[2] + soft_c
                inverse = lax.rsqrt(square)
                cube = inverse * inverse * inverse
                along = (gap[0] * at[3] + gap[1] * at[4] + gap[2] * at[5]) * cube
                plain = (square + soft_c) * cube
                new = [plain * at[3 + c] + gap[c] * along for c in range(3)]
                sums = new if sums is None else [a + b for a, b in zip(sums, new)]
            for c in range(3):
                partial_ref[pl.ds(chunk * 96 + c * LPTS + p, 1), :] = jnp.sum(
                    sums[c], axis=0, keepdims=True
                )
            return carry

        lax.fori_loop(0, LPTS, step, 0, unroll=16)

    same = (iota((LEAVES, LANES), 0) == lane_place()[0]).astype(F32).astype(BF16)
    same = jnp.concatenate([same] * 3, axis=1)
    partial = jnp.concatenate([partial_ref[k * 96 : (k + 1) * 96, :] for k in range(4)], axis=1)
    partial = jnp.concatenate(three(partial), axis=1).astype(BF16)
    by_leaf = [dot(same, partial[c * LPTS : (c + 1) * LPTS, :], NT) for c in range(3)]
    velocity = jnp.concatenate(by_leaf, axis=0) * (1.0 / EIGHT_PI)
    velocity = jnp.concatenate(three(velocity), axis=0).astype(BF16)
    node_row = iota((LPTS, DEVICES), 0)
    leaf_of = iota((LEAVES, DEVICES), 0)
    back_ref[...] = jnp.zeros_like(back_ref)
    slots, hots = [], []
    for r in range(CAP):
        entry = turned_ref[(REACH * CAP + r) * 8 : (REACH * CAP + r) * 8 + 8, :]
        slot = entry[6:7, :].astype(jnp.int32) - 1
        slots.append(slot)
        hots.append((node_row == (slot & (LPTS - 1))).astype(F32).astype(BF16))
    picked = thirds(dot(velocity, jnp.concatenate(hots, axis=1), NN), 3 * LEAVES)
    for r in range(CAP):
        mine = leaf_of == (slots[r] >> 5)
        for c in range(3):
            piece = picked[c * LEAVES : (c + 1) * LEAVES, r * 128 : (r + 1) * 128]
            back_ref[c * CAP + r : c * CAP + r + 1, :] = jnp.sum(
                jnp.where(mine, piece, 0.0), axis=0, keepdims=True
            )
    out_ref[...] = back_ref[...].T


def split_kernel(blocks_ref, out_ref):
    for i in range(2):
        out_ref[0, i], out_ref[1, i] = two(blocks_ref[i].T)


def fiber_kernel(
    arrived_ref, slot_ref, rank_ref, tension_ref, blocks_ref, out_ref, vector_ref
):
    hot = owner_hot(slot_ref[...]).astype(BF16)
    words = arrived_ref[...].T[: 3 * CAP]
    terms = jnp.concatenate(three(words), axis=0).astype(BF16)
    picked = thirds(dot(terms, hot, NN), 3 * CAP)
    here = iota((CAP, NODES), 0).astype(F32) == rank_ref[...]
    rows = [
        jnp.sum(jnp.where(here, picked[c * CAP : (c + 1) * CAP], 0.0), axis=0, keepdims=True)
        for c in range(3)
    ] + [tension_ref[...]]
    first = iota((1, 128), 1) < 64
    for pair in range(NODES // 128):
        cut = [row[:, pair * 128 : (pair + 1) * 128] for row in rows]
        swapped = [pltpu.roll(row, 64, 1) for row in cut]
        for k in range(2):
            a, b = cut[2 * k], cut[2 * k + 1]
            sa, sb = swapped[2 * k], swapped[2 * k + 1]
            lanes = slice(k * 128, (k + 1) * 128)
            vector_ref[2 * pair : 2 * pair + 1, lanes] = jnp.where(first, a, sb)
            vector_ref[2 * pair + 1 : 2 * pair + 2, lanes] = jnp.where(first, sa, b)
    vector = jnp.concatenate(two(vector_ref[...]), axis=0)
    row = iota((16, 256), 0) % 8
    total = jnp.zeros((16, 256), F32)
    for i in range(8):
        image = dot(vector, blocks_ref[0, i], NN) + dot(vector, blocks_ref[1, i], NN)
        total = jnp.where(row == i, image, total)
    out_ref[...] = total[:8] + total[8:]


def shape(*dims):
    return jax.ShapeDtypeStruct(dims, F32)


def shifted(value, by):
    pairs = [(i, i + by) for i in range(DEVICES) if 0 <= i + by < DEVICES]
    return lax.ppermute(value, AXES, pairs)


def grant(mib):
    return pltpu.CompilerParams(vmem_limit_bytes=mib << 20)


def exchange(rows):
    return lax.all_to_all(rows.reshape(-1), AXES, 0, 0, tiled=True).reshape(rows.shape)


def local(
    positions, forces, tension, node_slot, leaf_local, parent_local, l2l_maps, leaf_parent,
    leaf_octant, near_list, blocks,
):
    parent_local = parent_local.transpose(1, 0, 2)
    leaf_local = leaf_local.transpose(1, 0, 2)
    slot = node_slot.reshape(1, NODES)
    message, rank = pl.pallas_call(
        pack_kernel,
        out_shape=(shape(CHUNKS * 128, 128), shape(1, NODES)),
        scratch_shapes=[pltpu.VMEM((CHUNKS * 128, DEVICES), F32)],
        cost_estimate=pl.CostEstimate(flops=10**8, bytes_accessed=10**6, transcendentals=0),
        name="pack",
    )(positions, forces, slot)
    message, sent = lax.optimization_barrier((message, parent_local))
    arrived = exchange(message)
    from_before = shifted(sent, 1)
    from_after = shifted(sent, -1)

    vmem = pl.BlockSpec(memory_space=pltpu.VMEM)
    smem = pl.BlockSpec(memory_space=pltpu.SMEM)
    maps, near_hot, own_hot = pl.pallas_call(
        prepare_kernel,
        grid=(4,),
        out_shape=(
            jax.ShapeDtypeStruct((8, 384, 768), BF16),
            jax.ShapeDtypeStruct((LANES, LANES), BF16),
            jax.ShapeDtypeStruct((LANES, LANES), BF16),
        ),
        in_specs=[
            pl.BlockSpec((LEAVES, NEAR), lambda i: (0, 0)),
            pl.BlockSpec((2, 384, 384), lambda i: (i, 0, 0)),
        ],
        out_specs=(
            pl.BlockSpec((2, 384, 768), lambda i: (i, 0, 0)),
            pl.BlockSpec((128, LANES), lambda i: (i, 0)),
            pl.BlockSpec((128, LANES), lambda i: (i, 0)),
        ),
        scratch_shapes=[pltpu.VMEM((8, LANES), jnp.int32)],
        cost_estimate=pl.CostEstimate(flops=5 * 10**6, bytes_accessed=10**7, transcendentals=0),
        compiler_params=grant(8),
        name="prepare",
    )(near_list, l2l_maps)
    split = pl.pallas_call(
        split_kernel,
        grid=(4,),
        out_shape=jax.ShapeDtypeStruct((2, 8, 256, 256), BF16),
        in_specs=[pl.BlockSpec((2, 256, 256), lambda i: (i, 0, 0))],
        out_specs=pl.BlockSpec((2, 2, 256, 256), lambda i: (0, i, 0, 0)),
        cost_estimate=pl.CostEstimate(flops=2 * 10**6, bytes_accessed=4 * 10**6, transcendentals=0),
        compiler_params=grant(4),
        name="split",
    )(blocks)
    density = pl.pallas_call(
        density_kernel,
        out_shape=shape(3 * LPTS, 128),
        in_specs=[smem, smem, vmem, vmem, vmem, vmem, vmem],
        scratch_shapes=[
            pltpu.VMEM((24, NEQ), F32),
            pltpu.VMEM((LEAVES, 3 * NEQ), F32),
        ],
        cost_estimate=pl.CostEstimate(flops=10**9, bytes_accessed=5 * 10**6, transcendentals=0),
        compiler_params=grant(16),
        name="density",
    )(
        leaf_parent, leaf_octant, from_before, parent_local, from_after,
        leaf_local, maps,
    )
    back = pl.pallas_call(
        field_kernel,
        out_shape=shape(DEVICES, 128),
        scratch_shapes=[
            pltpu.VMEM((SPAN * CAP * 8, DEVICES), F32),
            pltpu.VMEM((1024, 128), F32),
            pltpu.VMEM((6 * LPTS, LANES), F32),
            pltpu.VMEM((12 * LPTS, 128), F32),
            pltpu.VMEM((12 * LPTS, 128), F32),
            pltpu.VMEM((128, DEVICES), F32),
        ],
        cost_estimate=pl.CostEstimate(flops=10**9, bytes_accessed=2 * 10**6, transcendentals=0),
        compiler_params=grant(16),
        name="field",
    )(arrived, near_hot, own_hot, density, jnp.asarray(shell_table()))
    returned = exchange(back)
    return pl.pallas_call(
        fiber_kernel,
        out_shape=shape(8, 256),
        scratch_shapes=[pltpu.VMEM((8, 256), F32)],
        cost_estimate=pl.CostEstimate(flops=10**8, bytes_accessed=2 * 10**6, transcendentals=0),
        compiler_params=grant(8),
        name="fiber",
    )(returned, slot, rank, tension.reshape(1, NODES), split)


def solution(mesh):
    both = ("aa", "ba")
    in_specs = (
        P(None, both), P(None, both), P(both), P(both), P(both, None, None), P(both, None, None),
        P(), P(both), P(both), P(both, None), P(both, None, None),
    )
    return jax.shard_map(
        local, mesh=mesh, in_specs=in_specs, out_specs=P(both, None), check_vma=False
    )
```

```python
import jax
import jax.numpy as jnp
import numpy as np
from jax import lax
from jax.experimental import pallas as pl
from jax.experimental.pallas import tpu as pltpu
from jax.sharding import PartitionSpec as P

DEVICES = 128
NODES = 512
CAP = 16
REACH = 8
SPAN = 2 * REACH + 1
LEAVES = 16
LPTS = 32
NEAR = 27
NEQ = 128
LANES = LEAVES * LPTS
GROUPS = NEQ // LPTS
FAR = GROUPS * LEAVES
WORDS = 7 * SPAN * CAP
CHUNKS = 15
EPS2 = 0.05**2
MARGIN = 0.05
SHELL = 2.95
GOLDEN = 2.399963229728653
EIGHT_PI = 25.132741228718345
AXES = ("aa", "ba")
HIGHEST = lax.Precision.HIGHEST
F32, BF16 = jnp.float32, jnp.bfloat16
NT = (((1,), (1,)), ((), ()))
NN = (((1,), (0,)), ((), ()))


def iota(shape, dim):
    return lax.broadcasted_iota(jnp.int32, shape, dim)


def three(x):
    high = x.astype(BF16).astype(F32)
    rest = x - high
    middle = rest.astype(BF16).astype(F32)
    return high, middle, rest - middle


def two(x):
    high = x.astype(BF16)
    return high, (x - high.astype(F32)).astype(BF16)


def dot(a, b, dims):
    return lax.dot_general(a, b, dims, preferred_element_type=F32)


def thirds(x, rows):
    return x[:rows] + x[rows : 2 * rows] + x[2 * rows :]


def shell_table():
    q = np.arange(NEQ, dtype=np.float32) + np.float32(0.5)
    h = (np.float32(1.0) - np.float32(2.0) * q / np.float32(NEQ)).astype(np.float32)
    radius = np.sqrt(np.maximum(np.float32(1.0) - h * h, 0)).astype(np.float32)
    angle = (q * np.float32(GOLDEN)).astype(np.float32)
    w = np.stack([radius * np.cos(angle), radius * np.sin(angle), h]).astype(np.float32)
    s = w / np.max(np.abs(w), axis=0, keepdims=True)
    table = np.zeros((3, LPTS, 128), np.float32)
    for g in range(GROUPS):
        table[:, :, g * LEAVES : (g + 1) * LEAVES] = s[:, g * LPTS : (g + 1) * LPTS, None]
    return table.reshape(3 * LPTS, 128)


def lane_place():
    lane = iota((1, LANES), 1)
    near = lane - FAR
    leaf = ((near.astype(F32) + 0.5) * (1.0 / NEAR)).astype(jnp.int32)
    place = near - leaf * NEAR
    is_near = (lane >= FAR) & (lane < FAR + LEAVES * NEAR)
    leaf = jnp.where(lane < FAR, lane & (LEAVES - 1), jnp.where(is_near, leaf, 0))
    return leaf, jnp.where(is_near, place, -1)


def device_index():
    return lax.axis_index("aa") * 16 + lax.axis_index("ba")


def owner_hot(slot):
    return (iota((DEVICES, NODES), 0) == (slot >> 9)).astype(F32)


def pack_kernel(pos_ref, force_ref, slot_ref, message_ref, rank_ref, rows_ref):
    slot = slot_ref[...]
    hot = owner_hot(slot)
    hot_b = hot.astype(BF16)
    row, column = iota((128, 256), 0), iota((128, 256), 1)
    before = ((row < column) | (column >= 128)).astype(F32).astype(BF16)
    earlier = jnp.zeros((DEVICES, 128), F32)
    ranks = []
    for k in range(NODES // 128):
        lanes = slice(k * 128, (k + 1) * 128)
        counts = dot(hot_b[:, lanes], before, NN)
        ranks.append(jnp.sum(hot[:, lanes] * (counts[:, :128] + earlier), axis=0, keepdims=True))
        earlier = earlier + counts[:, 128:]
    rank = jnp.concatenate(ranks, axis=1)
    rank_ref[...] = rank
    here = iota((CAP, NODES), 0).astype(F32) == rank
    within = (slot & (NODES - 1)).astype(F32) + 1.0
    payload = [pos_ref[c : c + 1, :] for c in range(3)]
    payload += [force_ref[c : c + 1, :] for c in range(3)] + [within]
    spread = jnp.concatenate([jnp.where(here, row, 0.0) for row in payload], axis=0)
    terms = jnp.concatenate(three(spread), axis=0).astype(BF16)
    buckets = thirds(dot(terms, hot_b, NT), 7 * CAP)
    rows_ref[WORDS:, :] = jnp.zeros((CHUNKS * 128 - WORDS, DEVICES), F32)
    for d in range(SPAN):
        shift = (REACH - d) % DEVICES
        moved = pltpu.roll(buckets, shift, 1) if shift else buckets
        rows_ref[d * 7 * CAP : (d + 1) * 7 * CAP, :] = moved
    for i in range(CHUNKS):
        message_ref[pl.ds(i, DEVICES, stride=CHUNKS), :] = rows_ref[i * 128 : (i + 1) * 128, :].T


def prepare_kernel(near_ref, local_ref, maps_ref, near_hot_ref, own_hot_ref, placed_ref, held_ref):
    held_ref[...] = maps_ref[...]
    leaf, place = lane_place()
    near = near_ref[...] - LEAVES * (device_index() - REACH)
    spread = (iota((NEAR, LANES), 0) == place).astype(F32).astype(BF16)
    own = iota((LEAVES, LANES), 0) == leaf
    values = jnp.concatenate([near & 3, near >> 2], axis=0).astype(F32).astype(BF16)
    values = dot(values, spread, NN)
    rows = []
    for k in range(2):
        value = jnp.where(own, values[k * LEAVES : (k + 1) * LEAVES], 0.0)
        value = jnp.sum(value, axis=0, keepdims=True).astype(jnp.int32)
        rows.append(jnp.where(place >= 0, value, -1))
    leaf_row = iota((128, LANES), 0)
    picks = ((near_hot_ref, *rows), (own_hot_ref, leaf & 3, (leaf + REACH * LEAVES) >> 2))
    for ref, quarter, row in picks:
        for w in range(4):
            here = leaf_row == jnp.where(quarter == w, row, -1)
            ref[w * 128 : (w + 1) * 128, :] = here.astype(F32).astype(BF16)
    group = iota((1, 128), 1) // LEAVES
    nothing = jnp.zeros((NEQ - FAR, NEQ), F32)
    for c in range(3):
        local = jnp.concatenate([local_ref[c]] * GROUPS + [nothing], axis=0).T
        placed = jnp.zeros((LPTS, 128), F32)
        for g in range(GROUPS):
            placed = jnp.where(group == g, local[g * LPTS : (g + 1) * LPTS], placed)
        placed_ref[c * LPTS : (c + 1) * LPTS, :] = placed


def density_kernel(
    parent_ref, octant_ref, before_ref, own_ref, after_ref, placed_ref, maps_ref, out_ref, six_ref
):
    first_parent = 2 * (device_index() - 1)
    for j in range(6):
        source = (before_ref, own_ref, after_ref)[j // 2]
        for c in range(3):
            six_ref[c * 8 + j : c * 8 + j + 1, :] = source[c, j % 2 : j % 2 + 1, :]
    out_ref[...] = jnp.zeros_like(out_ref)
    lane = iota((1, 128), 1)

    def translate(l, carry):
        octant, at = octant_ref[l], parent_ref[l] - first_parent
        parent = [six_ref[pl.ds(c * 8 + at, 1), :] for c in range(3)]
        for c in range(3):
            out = out_ref[c * LPTS : (c + 1) * LPTS, :]
            for g in range(GROUPS):
                rows = slice(c * NEQ + g * LPTS, c * NEQ + (g + 1) * LPTS)
                image = maps_ref[octant, rows, :NEQ] * parent[0]
                image = image + maps_ref[octant, rows, NEQ : 2 * NEQ] * parent[1]
                image = image + maps_ref[octant, rows, 2 * NEQ :] * parent[2]
                image = jnp.sum(image, axis=1, keepdims=True)
                out = jnp.where(lane == g * LEAVES + l, image, out)
            out_ref[c * LPTS : (c + 1) * LPTS, :] = out
        return carry

    lax.fori_loop(0, LEAVES, translate, 0, unroll=8)
    out_ref[...] += placed_ref[...]


def field_kernel(
    arrived_ref, near_hot_ref, own_hot_ref, density_ref, shell_ref, out_ref,
    turned_ref, tree_ref, source_ref, target_ref, partial_ref, back_ref,
):
    turned = [arrived_ref[pl.ds(i, DEVICES, stride=CHUNKS), :].T for i in range(CHUNKS)]
    tree_ref[SPAN * 32 :, :] = jnp.zeros((1024 - SPAN * 32, 128), F32)
    low_row = iota((128, 128), 0).astype(F32).astype(BF16)
    half_row = [(iota((16, 128), 0) // 8 + k).astype(F32).astype(BF16) for k in (0, 2)]
    one, zero = jnp.ones((16, 128), BF16), jnp.zeros((16, 128), BF16)

    def narrow(row):
        return jnp.broadcast_to(row.astype(F32), (16, 128)).astype(BF16)

    def place(d):
        lows, values = [], []
        for r in range(CAP):
            entry = turned_ref[(d * CAP + r) * 8 : (d * CAP + r) * 8 + 8, :]
            slot = entry[6:7, :].astype(jnp.int32) - 1
            low, high = narrow(slot & 127), narrow(slot >> 7)
            lows.append(
                jnp.concatenate(
                    [jnp.where(low_row[k : k + 16] == low, one, zero) for k in range(0, 128, 16)],
                    axis=0,
                )
            )
            here = [row == high for row in half_row]
            parts = [jnp.concatenate([part, part], axis=0).astype(BF16) for part in three(entry)]
            values.append(
                jnp.concatenate([jnp.where(h, part, zero) for part in parts for h in here], axis=0)
            )
        placed = dot(jnp.concatenate(lows, axis=1), jnp.concatenate(values, axis=1), NT).T
        tree_ref[d * 32 : (d + 1) * 32, :] = thirds(placed, 32)

    for d in range(SPAN):
        for c in range(7):
            at = d * 7 * CAP + c * CAP
            turned_ref[pl.ds(d * 8 * CAP + c, CAP, stride=8), :] = turned[at // 128][
                at % 128 : at % 128 + CAP, :
            ]
        turned_ref[pl.ds(d * 8 * CAP + 7, CAP, stride=8), :] = jnp.zeros((CAP, DEVICES), F32)
        place(d)

    terms = [[], [], []]
    for c in range(6):
        turned_c = tree_ref[pl.ds(c, 128, stride=8), :].T
        for s, part in enumerate(three(turned_c)):
            part = part.astype(BF16)
            terms[s].append(
                jnp.concatenate([part[w * LPTS : (w + 1) * LPTS] for w in range(4)], axis=1)
            )
    everything = jnp.concatenate([t for s in range(3) for t in terms[s]], axis=0)
    positions = jnp.concatenate([t for s in range(3) for t in terms[s][:3]], axis=0)
    gathered = thirds(dot(everything, near_hot_ref[...], NN), 6 * LPTS)
    targets = thirds(dot(positions, own_hot_ref[...], NN), 3 * LPTS)
    for k in range(LANES // 128):
        target_ref[k * 96 : (k + 1) * 96, :] = targets[:, k * 128 : (k + 1) * 128]
    axes = [targets[c * LPTS : (c + 1) * LPTS] for c in range(3)]
    centers = [jnp.sum(a, axis=0, keepdims=True) * (1.0 / LPTS) for a in axes]
    half = jnp.maximum(
        jnp.maximum(
            jnp.max(jnp.abs(axes[0] - centers[0]), axis=0, keepdims=True),
            jnp.max(jnp.abs(axes[1] - centers[1]), axis=0, keepdims=True),
        ),
        jnp.max(jnp.abs(axes[2] - centers[2]), axis=0, keepdims=True),
    ) + MARGIN
    for c in range(3):
        rows = slice(c * LPTS, (c + 1) * LPTS)
        more = slice((3 + c) * LPTS, (4 + c) * LPTS)
        first = gathered[rows, :128] + (SHELL * half[:, :128]) * shell_ref[rows, :]
        source_ref[rows, :128] = first + jnp.where(iota((1, 128), 1) < FAR, centers[c][:, :128], 0.0)
        source_ref[rows, 128:] = gathered[rows, 128:]
        source_ref[more, :128] = gathered[more, :128] + density_ref[rows, :]
        source_ref[more, 128:] = gathered[more, 128:]
    soft = jnp.where(iota((1, LANES), 1) < FAR, 0.0, EPS2)
    for chunk in range(LANES // 128):
        lanes = slice(chunk * 128, (chunk + 1) * 128)
        soft_c = soft[:, lanes]

        def step(p, carry):
            aim = [target_ref[pl.ds(chunk * 96 + c * LPTS + p, 1), :] for c in range(3)]
            sums = None
            for g in range(LPTS // 8):
                at = [source_ref[c * LPTS + g * 8 : c * LPTS + g * 8 + 8, lanes] for c in range(6)]
                gap = [aim[c] - at[c] for c in range(3)]
                square = gap[0] * gap[0] + gap[1] * gap[1] + gap[2] * gap[2] + soft_c
                inverse = lax.rsqrt(square)
                cube = inverse * inverse * inverse
                along = (gap[0] * at[3] + gap[1] * at[4] + gap[2] * at[5]) * cube
                plain = (square + soft_c) * cube
                new = [plain * at[3 + c] + gap[c] * along for c in range(3)]
                sums = new if sums is None else [a + b for a, b in zip(sums, new)]
            for c in range(3):
                partial_ref[pl.ds(chunk * 96 + c * LPTS + p, 1), :] = jnp.sum(
                    sums[c], axis=0, keepdims=True
                )
            return carry

        lax.fori_loop(0, LPTS, step, 0, unroll=16)

    same = (iota((LEAVES, LANES), 0) == lane_place()[0]).astype(F32).astype(BF16)
    same = jnp.concatenate([same] * 3, axis=1)
    partial = jnp.concatenate([partial_ref[k * 96 : (k + 1) * 96, :] for k in range(4)], axis=1)
    partial = jnp.concatenate(three(partial), axis=1).astype(BF16)
    by_leaf = [dot(same, partial[c * LPTS : (c + 1) * LPTS, :], NT) for c in range(3)]
    velocity = jnp.concatenate(by_leaf, axis=0) * (1.0 / EIGHT_PI)
    velocity = jnp.concatenate(three(velocity), axis=0).astype(BF16)
    node_row = iota((LPTS, DEVICES), 0)
    leaf_of = iota((LEAVES, DEVICES), 0)
    back_ref[...] = jnp.zeros_like(back_ref)
    slots, hots = [], []
    for r in range(CAP):
        entry = turned_ref[(REACH * CAP + r) * 8 : (REACH * CAP + r) * 8 + 8, :]
        slot = entry[6:7, :].astype(jnp.int32) - 1
        slots.append(slot)
        hots.append((node_row == (slot & (LPTS - 1))).astype(F32).astype(BF16))
    picked = thirds(dot(velocity, jnp.concatenate(hots, axis=1), NN), 3 * LEAVES)
    for r in range(CAP):
        mine = leaf_of == (slots[r] >> 5)
        for c in range(3):
            piece = picked[c * LEAVES : (c + 1) * LEAVES, r * 128 : (r + 1) * 128]
            back_ref[c * CAP + r : c * CAP + r + 1, :] = jnp.sum(
                jnp.where(mine, piece, 0.0), axis=0, keepdims=True
            )
    out_ref[...] = back_ref[...].T


def split_kernel(blocks_ref, out_ref):
    for i in range(2):
        out_ref[0, i], out_ref[1, i] = two(blocks_ref[i].T)


def fiber_kernel(
    arrived_ref, slot_ref, rank_ref, tension_ref, blocks_ref, out_ref, vector_ref
):
    hot = owner_hot(slot_ref[...]).astype(BF16)
    words = arrived_ref[...].T[: 3 * CAP]
    terms = jnp.concatenate(three(words), axis=0).astype(BF16)
    picked = thirds(dot(terms, hot, NN), 3 * CAP)
    here = iota((CAP, NODES), 0).astype(F32) == rank_ref[...]
    rows = [
        jnp.sum(jnp.where(here, picked[c * CAP : (c + 1) * CAP], 0.0), axis=0, keepdims=True)
        for c in range(3)
    ] + [tension_ref[...]]
    first = iota((1, 128), 1) < 64
    for pair in range(NODES // 128):
        cut = [row[:, pair * 128 : (pair + 1) * 128] for row in rows]
        swapped = [pltpu.roll(row, 64, 1) for row in cut]
        for k in range(2):
            a, b = cut[2 * k], cut[2 * k + 1]
            sa, sb = swapped[2 * k], swapped[2 * k + 1]
            lanes = slice(k * 128, (k + 1) * 128)
            vector_ref[2 * pair : 2 * pair + 1, lanes] = jnp.where(first, a, sb)
            vector_ref[2 * pair + 1 : 2 * pair + 2, lanes] = jnp.where(first, sa, b)
    vector = jnp.concatenate(two(vector_ref[...]), axis=0)
    row = iota((16, 256), 0) % 8
    total = jnp.zeros((16, 256), F32)
    for i in range(8):
        image = dot(vector, blocks_ref[0, i], NN) + dot(vector, blocks_ref[1, i], NN)
        total = jnp.where(row == i, image, total)
    out_ref[...] = total[:8] + total[8:]


def shape(*dims):
    return jax.ShapeDtypeStruct(dims, F32)


def shifted(value, by):
    pairs = [(i, i + by) for i in range(DEVICES) if 0 <= i + by < DEVICES]
    return lax.ppermute(value, AXES, pairs)


def grant(mib):
    return pltpu.CompilerParams(vmem_limit_bytes=mib << 20)


def exchange(rows):
    return lax.all_to_all(rows.reshape(-1), AXES, 0, 0, tiled=True).reshape(rows.shape)


def local(
    positions, forces, tension, node_slot, leaf_local, parent_local, l2l_maps, leaf_parent,
    leaf_octant, near_list, blocks,
):
    parent_local = parent_local.transpose(1, 0, 2)
    leaf_local = leaf_local.transpose(1, 0, 2)
    slot = node_slot.reshape(1, NODES)
    message, rank = pl.pallas_call(
        pack_kernel,
        out_shape=(shape(CHUNKS * 128, 128), shape(1, NODES)),
        scratch_shapes=[pltpu.VMEM((CHUNKS * 128, DEVICES), F32)],
        cost_estimate=pl.CostEstimate(flops=10**8, bytes_accessed=10**6, transcendentals=0),
        name="pack",
    )(positions, forces, slot)
    message, sent = lax.optimization_barrier((message, parent_local))
    arrived = exchange(message)
    from_before = shifted(sent, 1)
    from_after = shifted(sent, -1)

    vmem = pl.BlockSpec(memory_space=pltpu.VMEM)
    smem = pl.BlockSpec(memory_space=pltpu.SMEM)
    near_hot, own_hot, placed, maps = pl.pallas_call(
        prepare_kernel,
        out_shape=(
            jax.ShapeDtypeStruct((LANES, LANES), BF16),
            jax.ShapeDtypeStruct((LANES, LANES), BF16),
            shape(3 * LPTS, 128),
            shape(8, 3 * NEQ, 3 * NEQ),
        ),
        cost_estimate=pl.CostEstimate(flops=5 * 10**6, bytes_accessed=10**7, transcendentals=0),
        compiler_params=grant(8),
        name="prepare",
    )(near_list, leaf_local, l2l_maps)
    split = pl.pallas_call(
        split_kernel,
        grid=(4,),
        out_shape=jax.ShapeDtypeStruct((2, 8, 256, 256), BF16),
        in_specs=[pl.BlockSpec((2, 256, 256), lambda i: (i, 0, 0))],
        out_specs=pl.BlockSpec((2, 2, 256, 256), lambda i: (0, i, 0, 0)),
        cost_estimate=pl.CostEstimate(flops=2 * 10**6, bytes_accessed=4 * 10**6, transcendentals=0),
        compiler_params=grant(4),
        name="split",
    )(blocks)
    density = pl.pallas_call(
        density_kernel,
        out_shape=shape(3 * LPTS, 128),
        in_specs=[smem, smem, vmem, vmem, vmem, vmem, vmem],
        scratch_shapes=[pltpu.VMEM((24, NEQ), F32)],
        cost_estimate=pl.CostEstimate(flops=10**9, bytes_accessed=5 * 10**6, transcendentals=0),
        compiler_params=grant(16),
        name="density",
    )(
        leaf_parent, leaf_octant, from_before, parent_local, from_after,
        placed, maps,
    )
    back = pl.pallas_call(
        field_kernel,
        out_shape=shape(DEVICES, 128),
        scratch_shapes=[
            pltpu.VMEM((SPAN * CAP * 8, DEVICES), F32),
            pltpu.VMEM((1024, 128), F32),
            pltpu.VMEM((6 * LPTS, LANES), F32),
            pltpu.VMEM((12 * LPTS, 128), F32),
            pltpu.VMEM((12 * LPTS, 128), F32),
            pltpu.VMEM((128, DEVICES), F32),
        ],
        cost_estimate=pl.CostEstimate(flops=10**9, bytes_accessed=2 * 10**6, transcendentals=0),
        compiler_params=grant(16),
        name="field",
    )(arrived, near_hot, own_hot, density, jnp.asarray(shell_table()))
    returned = exchange(back)
    return pl.pallas_call(
        fiber_kernel,
        out_shape=shape(8, 256),
        scratch_shapes=[pltpu.VMEM((8, 256), F32)],
        cost_estimate=pl.CostEstimate(flops=10**8, bytes_accessed=2 * 10**6, transcendentals=0),
        compiler_params=grant(8),
        name="fiber",
    )(returned, slot, rank, tension.reshape(1, NODES), split)


def solution(mesh):
    both = ("aa", "ba")
    in_specs = (
        P(None, both), P(None, both), P(both), P(both), P(both, None, None), P(both, None, None),
        P(), P(both), P(both), P(both, None), P(both, None, None),
    )
    return jax.shard_map(
        local, mesh=mesh, in_specs=in_specs, out_specs=P(both, None), check_vma=False
    )
```

```python
import jax
import jax.numpy as jnp
import numpy as np
from jax import lax
from jax.experimental import pallas as pl
from jax.experimental.pallas import tpu as pltpu
from jax.sharding import PartitionSpec as P

DEVICES = 128
NODES = 512
CAP = 16
REACH = 8
SPAN = 2 * REACH + 1
LEAVES = 16
LPTS = 32
NEAR = 27
NEQ = 128
LANES = LEAVES * LPTS
GROUPS = NEQ // LPTS
FAR = GROUPS * LEAVES
WORDS = 7 * SPAN * CAP
CHUNKS = 15
EPS2 = 0.05**2
MARGIN = 0.05
SHELL = 2.95
GOLDEN = 2.399963229728653
EIGHT_PI = 25.132741228718345
AXES = ("aa", "ba")
HIGHEST = lax.Precision.HIGHEST
F32, BF16 = jnp.float32, jnp.bfloat16
NT = (((1,), (1,)), ((), ()))
NN = (((1,), (0,)), ((), ()))


def iota(shape, dim):
    return lax.broadcasted_iota(jnp.int32, shape, dim)


def three(x):
    high = x.astype(BF16).astype(F32)
    rest = x - high
    middle = rest.astype(BF16).astype(F32)
    return high, middle, rest - middle


def two(x):
    high = x.astype(BF16)
    return high, (x - high.astype(F32)).astype(BF16)


def dot(a, b, dims):
    return lax.dot_general(a, b, dims, preferred_element_type=F32)


def thirds(x, rows):
    return x[:rows] + x[rows : 2 * rows] + x[2 * rows :]


def shell_table():
    q = np.arange(NEQ, dtype=np.float32) + np.float32(0.5)
    h = (np.float32(1.0) - np.float32(2.0) * q / np.float32(NEQ)).astype(np.float32)
    radius = np.sqrt(np.maximum(np.float32(1.0) - h * h, 0)).astype(np.float32)
    angle = (q * np.float32(GOLDEN)).astype(np.float32)
    w = np.stack([radius * np.cos(angle), radius * np.sin(angle), h]).astype(np.float32)
    s = w / np.max(np.abs(w), axis=0, keepdims=True)
    table = np.zeros((3, LPTS, 128), np.float32)
    for g in range(GROUPS):
        table[:, :, g * LEAVES : (g + 1) * LEAVES] = s[:, g * LPTS : (g + 1) * LPTS, None]
    return table.reshape(3 * LPTS, 128)


def lane_place():
    lane = iota((1, LANES), 1)
    near = lane - FAR
    leaf = ((near.astype(F32) + 0.5) * (1.0 / NEAR)).astype(jnp.int32)
    place = near - leaf * NEAR
    is_near = (lane >= FAR) & (lane < FAR + LEAVES * NEAR)
    leaf = jnp.where(lane < FAR, lane & (LEAVES - 1), jnp.where(is_near, leaf, 0))
    return leaf, jnp.where(is_near, place, -1)


def device_index():
    return lax.axis_index("aa") * 16 + lax.axis_index("ba")


def owner_hot(slot):
    return (iota((DEVICES, NODES), 0) == (slot >> 9)).astype(F32)


def pack_kernel(pos_ref, force_ref, slot_ref, message_ref, rank_ref, rows_ref):
    slot = slot_ref[...]
    hot = owner_hot(slot)
    hot_b = hot.astype(BF16)
    row, column = iota((128, 256), 0), iota((128, 256), 1)
    before = ((row < column) | (column >= 128)).astype(F32).astype(BF16)
    earlier = jnp.zeros((DEVICES, 128), F32)
    ranks = []
    for k in range(NODES // 128):
        lanes = slice(k * 128, (k + 1) * 128)
        counts = dot(hot_b[:, lanes], before, NN)
        ranks.append(jnp.sum(hot[:, lanes] * (counts[:, :128] + earlier), axis=0, keepdims=True))
        earlier = earlier + counts[:, 128:]
    rank = jnp.concatenate(ranks, axis=1)
    rank_ref[...] = rank
    here = iota((CAP, NODES), 0).astype(F32) == rank
    within = (slot & (NODES - 1)).astype(F32) + 1.0
    payload = [pos_ref[c : c + 1, :] for c in range(3)]
    payload += [force_ref[c : c + 1, :] for c in range(3)] + [within]
    spread = jnp.concatenate([jnp.where(here, row, 0.0) for row in payload], axis=0)
    terms = jnp.concatenate(three(spread), axis=0).astype(BF16)
    buckets = thirds(dot(terms, hot_b, NT), 7 * CAP)
    rows_ref[WORDS:, :] = jnp.zeros((CHUNKS * 128 - WORDS, DEVICES), F32)
    for d in range(SPAN):
        shift = (REACH - d) % DEVICES
        moved = pltpu.roll(buckets, shift, 1) if shift else buckets
        rows_ref[d * 7 * CAP : (d + 1) * 7 * CAP, :] = moved
    for i in range(CHUNKS):
        message_ref[pl.ds(i, DEVICES, stride=CHUNKS), :] = rows_ref[i * 128 : (i + 1) * 128, :].T


def prepare_kernel(near_ref, local_ref, maps_ref, near_hot_ref, own_hot_ref, placed_ref, held_ref):
    held_ref[...] = maps_ref[...]
    leaf, place = lane_place()
    near = near_ref[...] - LEAVES * (device_index() - REACH)
    spread = (iota((NEAR, LANES), 0) == place).astype(F32).astype(BF16)
    own = iota((LEAVES, LANES), 0) == leaf
    values = jnp.concatenate([near & 3, near >> 2], axis=0).astype(F32).astype(BF16)
    values = dot(values, spread, NN)
    rows = []
    for k in range(2):
        value = jnp.where(own, values[k * LEAVES : (k + 1) * LEAVES], 0.0)
        value = jnp.sum(value, axis=0, keepdims=True).astype(jnp.int32)
        rows.append(jnp.where(place >= 0, value, -1))
    leaf_row = iota((128, LANES), 0)
    picks = ((near_hot_ref, *rows), (own_hot_ref, leaf & 3, (leaf + REACH * LEAVES) >> 2))
    for ref, quarter, row in picks:
        for w in range(4):
            here = leaf_row == jnp.where(quarter == w, row, -1)
            ref[w * 128 : (w + 1) * 128, :] = here.astype(F32).astype(BF16)
    group = iota((1, 128), 1) // LEAVES
    nothing = jnp.zeros((NEQ - FAR, NEQ), F32)
    for c in range(3):
        local = jnp.concatenate([local_ref[c]] * GROUPS + [nothing], axis=0).T
        placed = jnp.zeros((LPTS, 128), F32)
        for g in range(GROUPS):
            placed = jnp.where(group == g, local[g * LPTS : (g + 1) * LPTS], placed)
        placed_ref[c * LPTS : (c + 1) * LPTS, :] = placed


def density_kernel(
    parent_ref, octant_ref, before_ref, own_ref, after_ref, placed_ref, maps_ref, out_ref, six_ref
):
    first_parent = 2 * (device_index() - 1)
    for j in range(6):
        source = (before_ref, own_ref, after_ref)[j // 2]
        for c in range(3):
            six_ref[c * 8 + j : c * 8 + j + 1, :] = source[c, j % 2 : j % 2 + 1, :]
    out_ref[...] = jnp.zeros_like(out_ref)
    lane = iota((1, 128), 1)

    def translate(l, carry):
        octant, at = octant_ref[l], parent_ref[l] - first_parent
        parent = [six_ref[pl.ds(c * 8 + at, 1), :] for c in range(3)]
        for c in range(3):
            out = out_ref[c * LPTS : (c + 1) * LPTS, :]
            for g in range(GROUPS):
                rows = slice(c * NEQ + g * LPTS, c * NEQ + (g + 1) * LPTS)
                image = maps_ref[octant, rows, :NEQ] * parent[0]
                image = image + maps_ref[octant, rows, NEQ : 2 * NEQ] * parent[1]
                image = image + maps_ref[octant, rows, 2 * NEQ :] * parent[2]
                image = jnp.sum(image, axis=1, keepdims=True)
                out = jnp.where(lane == g * LEAVES + l, image, out)
            out_ref[c * LPTS : (c + 1) * LPTS, :] = out
        return carry

    lax.fori_loop(0, LEAVES, translate, 0, unroll=True)
    out_ref[...] += placed_ref[...]


def field_kernel(
    arrived_ref, near_hot_ref, own_hot_ref, density_ref, shell_ref, out_ref,
    turned_ref, tree_ref, source_ref, target_ref, partial_ref, back_ref,
):
    turned = [arrived_ref[pl.ds(i, DEVICES, stride=CHUNKS), :].T for i in range(CHUNKS)]
    tree_ref[SPAN * 32 :, :] = jnp.zeros((1024 - SPAN * 32, 128), F32)
    low_row = iota((128, 128), 0).astype(F32).astype(BF16)
    half_row = [(iota((16, 128), 0) // 8 + k).astype(F32).astype(BF16) for k in (0, 2)]
    one, zero = jnp.ones((16, 128), BF16), jnp.zeros((16, 128), BF16)

    def narrow(row):
        return jnp.broadcast_to(row.astype(F32), (16, 128)).astype(BF16)

    def place(d):
        lows, values = [], []
        for r in range(CAP):
            entry = turned_ref[(d * CAP + r) * 8 : (d * CAP + r) * 8 + 8, :]
            slot = entry[6:7, :].astype(jnp.int32) - 1
            low, high = narrow(slot & 127), narrow(slot >> 7)
            lows.append(
                jnp.concatenate(
                    [jnp.where(low_row[k : k + 16] == low, one, zero) for k in range(0, 128, 16)],
                    axis=0,
                )
            )
            here = [row == high for row in half_row]
            parts = [jnp.concatenate([part, part], axis=0).astype(BF16) for part in three(entry)]
            values.append(
                jnp.concatenate([jnp.where(h, part, zero) for part in parts for h in here], axis=0)
            )
        placed = dot(jnp.concatenate(lows, axis=1), jnp.concatenate(values, axis=1), NT).T
        tree_ref[d * 32 : (d + 1) * 32, :] = thirds(placed, 32)

    for d in range(SPAN):
        for c in range(7):
            at = d * 7 * CAP + c * CAP
            turned_ref[pl.ds(d * 8 * CAP + c, CAP, stride=8), :] = turned[at // 128][
                at % 128 : at % 128 + CAP, :
            ]
        turned_ref[pl.ds(d * 8 * CAP + 7, CAP, stride=8), :] = jnp.zeros((CAP, DEVICES), F32)
        place(d)

    terms = [[], [], []]
    for c in range(6):
        turned_c = tree_ref[pl.ds(c, 128, stride=8), :].T
        for s, part in enumerate(three(turned_c)):
            part = part.astype(BF16)
            terms[s].append(
                jnp.concatenate([part[w * LPTS : (w + 1) * LPTS] for w in range(4)], axis=1)
            )
    everything = jnp.concatenate([t for s in range(3) for t in terms[s]], axis=0)
    positions = jnp.concatenate([t for s in range(3) for t in terms[s][:3]], axis=0)
    gathered = thirds(dot(everything, near_hot_ref[...], NN), 6 * LPTS)
    targets = thirds(dot(positions, own_hot_ref[...], NN), 3 * LPTS)
    for k in range(LANES // 128):
        target_ref[k * 96 : (k + 1) * 96, :] = targets[:, k * 128 : (k + 1) * 128]
    axes = [targets[c * LPTS : (c + 1) * LPTS] for c in range(3)]
    centers = [jnp.sum(a, axis=0, keepdims=True) * (1.0 / LPTS) for a in axes]
    half = jnp.maximum(
        jnp.maximum(
            jnp.max(jnp.abs(axes[0] - centers[0]), axis=0, keepdims=True),
            jnp.max(jnp.abs(axes[1] - centers[1]), axis=0, keepdims=True),
        ),
        jnp.max(jnp.abs(axes[2] - centers[2]), axis=0, keepdims=True),
    ) + MARGIN
    for c in range(3):
        rows = slice(c * LPTS, (c + 1) * LPTS)
        more = slice((3 + c) * LPTS, (4 + c) * LPTS)
        first = gathered[rows, :128] + (SHELL * half[:, :128]) * shell_ref[rows, :]
        source_ref[rows, :128] = first + jnp.where(iota((1, 128), 1) < FAR, centers[c][:, :128], 0.0)
        source_ref[rows, 128:] = gathered[rows, 128:]
        source_ref[more, :128] = gathered[more, :128] + density_ref[rows, :]
        source_ref[more, 128:] = gathered[more, 128:]
    soft = jnp.where(iota((1, LANES), 1) < FAR, 0.0, EPS2)
    for chunk in range(LANES // 128):
        lanes = slice(chunk * 128, (chunk + 1) * 128)
        soft_c = soft[:, lanes]

        def step(i, carry):
            first = i * 8
            sums = [None] * 8
            aims = [
                [target_ref[pl.ds(chunk * 96 + c * LPTS + first + k, 1), :] for c in range(3)]
                for k in range(8)
            ]
            for g in range(LPTS // 8):
                at = [source_ref[c * LPTS + g * 8 : c * LPTS + g * 8 + 8, lanes] for c in range(6)]
                for k in range(8):
                    gap = [aims[k][c] - at[c] for c in range(3)]
                    square = gap[0] * gap[0] + gap[1] * gap[1] + gap[2] * gap[2] + soft_c
                    inverse = lax.rsqrt(square)
                    cube = inverse * inverse * inverse
                    along = (gap[0] * at[3] + gap[1] * at[4] + gap[2] * at[5]) * cube
                    plain = (square + soft_c) * cube
                    new = [plain * at[3 + c] + gap[c] * along for c in range(3)]
                    sums[k] = new if sums[k] is None else [a + b for a, b in zip(sums[k], new)]
            for k in range(8):
                for c in range(3):
                    partial_ref[pl.ds(chunk * 96 + c * LPTS + first + k, 1), :] = jnp.sum(
                        sums[k][c], axis=0, keepdims=True
                    )
            return carry

        lax.fori_loop(0, LPTS // 8, step, 0, unroll=2)

    same = (iota((LEAVES, LANES), 0) == lane_place()[0]).astype(F32).astype(BF16)
    same = jnp.concatenate([same] * 3, axis=1)
    partial = jnp.concatenate([partial_ref[k * 96 : (k + 1) * 96, :] for k in range(4)], axis=1)
    partial = jnp.concatenate(three(partial), axis=1).astype(BF16)
    by_leaf = [dot(same, partial[c * LPTS : (c + 1) * LPTS, :], NT) for c in range(3)]
    velocity = jnp.concatenate(by_leaf, axis=0) * (1.0 / EIGHT_PI)
    velocity = jnp.concatenate(three(velocity), axis=0).astype(BF16)
    node_row = iota((LPTS, DEVICES), 0)
    leaf_of = iota((LEAVES, DEVICES), 0)
    back_ref[...] = jnp.zeros_like(back_ref)
    slots, hots = [], []
    for r in range(CAP):
        entry = turned_ref[(REACH * CAP + r) * 8 : (REACH * CAP + r) * 8 + 8, :]
        slot = entry[6:7, :].astype(jnp.int32) - 1
        slots.append(slot)
        hots.append((node_row == (slot & (LPTS - 1))).astype(F32).astype(BF16))
    picked = thirds(dot(velocity, jnp.concatenate(hots, axis=1), NN), 3 * LEAVES)
    for r in range(CAP):
        mine = leaf_of == (slots[r] >> 5)
        for c in range(3):
            piece = picked[c * LEAVES : (c + 1) * LEAVES, r * 128 : (r + 1) * 128]
            back_ref[c * CAP + r : c * CAP + r + 1, :] = jnp.sum(
                jnp.where(mine, piece, 0.0), axis=0, keepdims=True
            )
    out_ref[...] = back_ref[...].T


def split_kernel(blocks_ref, out_ref):
    for i in range(2):
        out_ref[0, i], out_ref[1, i] = two(blocks_ref[i].T)


def fiber_kernel(
    arrived_ref, slot_ref, rank_ref, tension_ref, blocks_ref, out_ref, vector_ref
):
    hot = owner_hot(slot_ref[...]).astype(BF16)
    words = arrived_ref[...].T[: 3 * CAP]
    terms = jnp.concatenate(three(words), axis=0).astype(BF16)
    picked = thirds(dot(terms, hot, NN), 3 * CAP)
    here = iota((CAP, NODES), 0).astype(F32) == rank_ref[...]
    rows = [
        jnp.sum(jnp.where(here, picked[c * CAP : (c + 1) * CAP], 0.0), axis=0, keepdims=True)
        for c in range(3)
    ] + [tension_ref[...]]
    first = iota((1, 128), 1) < 64
    for pair in range(NODES // 128):
        cut = [row[:, pair * 128 : (pair + 1) * 128] for row in rows]
        swapped = [pltpu.roll(row, 64, 1) for row in cut]
        for k in range(2):
            a, b = cut[2 * k], cut[2 * k + 1]
            sa, sb = swapped[2 * k], swapped[2 * k + 1]
            lanes = slice(k * 128, (k + 1) * 128)
            vector_ref[2 * pair : 2 * pair + 1, lanes] = jnp.where(first, a, sb)
            vector_ref[2 * pair + 1 : 2 * pair + 2, lanes] = jnp.where(first, sa, b)
    vector = jnp.concatenate(two(vector_ref[...]), axis=0)
    row = iota((16, 256), 0) % 8
    total = jnp.zeros((16, 256), F32)
    for i in range(8):
        image = dot(vector, blocks_ref[0, i], NN) + dot(vector, blocks_ref[1, i], NN)
        total = jnp.where(row == i, image, total)
    out_ref[...] = total[:8] + total[8:]


def shape(*dims):
    return jax.ShapeDtypeStruct(dims, F32)


def shifted(value, by):
    pairs = [(i, i + by) for i in range(DEVICES) if 0 <= i + by < DEVICES]
    return lax.ppermute(value, AXES, pairs)


def grant(mib):
    return pltpu.CompilerParams(vmem_limit_bytes=mib << 20)


def exchange(rows):
    return lax.all_to_all(rows.reshape(-1), AXES, 0, 0, tiled=True).reshape(rows.shape)


def local(
    positions, forces, tension, node_slot, leaf_local, parent_local, l2l_maps, leaf_parent,
    leaf_octant, near_list, blocks,
):
    parent_local = parent_local.transpose(1, 0, 2)
    leaf_local = leaf_local.transpose(1, 0, 2)
    slot = node_slot.reshape(1, NODES)
    message, rank = pl.pallas_call(
        pack_kernel,
        out_shape=(shape(CHUNKS * 128, 128), shape(1, NODES)),
        scratch_shapes=[pltpu.VMEM((CHUNKS * 128, DEVICES), F32)],
        cost_estimate=pl.CostEstimate(flops=10**8, bytes_accessed=10**6, transcendentals=0),
        name="pack",
    )(positions, forces, slot)
    message, sent = lax.optimization_barrier((message, parent_local))
    arrived = exchange(message)
    from_before = shifted(sent, 1)
    from_after = shifted(sent, -1)

    vmem = pl.BlockSpec(memory_space=pltpu.VMEM)
    smem = pl.BlockSpec(memory_space=pltpu.SMEM)
    near_hot, own_hot, placed, maps = pl.pallas_call(
        prepare_kernel,
        out_shape=(
            jax.ShapeDtypeStruct((LANES, LANES), BF16),
            jax.ShapeDtypeStruct((LANES, LANES), BF16),
            shape(3 * LPTS, 128),
            shape(8, 3 * NEQ, 3 * NEQ),
        ),
        cost_estimate=pl.CostEstimate(flops=5 * 10**6, bytes_accessed=10**7, transcendentals=0),
        compiler_params=grant(8),
        name="prepare",
    )(near_list, leaf_local, l2l_maps)
    split = pl.pallas_call(
        split_kernel,
        grid=(4,),
        out_shape=jax.ShapeDtypeStruct((2, 8, 256, 256), BF16),
        in_specs=[pl.BlockSpec((2, 256, 256), lambda i: (i, 0, 0))],
        out_specs=pl.BlockSpec((2, 2, 256, 256), lambda i: (0, i, 0, 0)),
        cost_estimate=pl.CostEstimate(flops=2 * 10**6, bytes_accessed=4 * 10**6, transcendentals=0),
        compiler_params=grant(4),
        name="split",
    )(blocks)
    density = pl.pallas_call(
        density_kernel,
        out_shape=shape(3 * LPTS, 128),
        in_specs=[smem, smem, vmem, vmem, vmem, vmem, vmem],
        scratch_shapes=[pltpu.VMEM((24, NEQ), F32)],
        cost_estimate=pl.CostEstimate(flops=10**9, bytes_accessed=5 * 10**6, transcendentals=0),
        compiler_params=grant(16),
        name="density",
    )(
        leaf_parent, leaf_octant, from_before, parent_local, from_after,
        placed, maps,
    )
    back = pl.pallas_call(
        field_kernel,
        out_shape=shape(DEVICES, 128),
        scratch_shapes=[
            pltpu.VMEM((SPAN * CAP * 8, DEVICES), F32),
            pltpu.VMEM((1024, 128), F32),
            pltpu.VMEM((6 * LPTS, LANES), F32),
            pltpu.VMEM((12 * LPTS, 128), F32),
            pltpu.VMEM((12 * LPTS, 128), F32),
            pltpu.VMEM((128, DEVICES), F32),
        ],
        cost_estimate=pl.CostEstimate(flops=10**9, bytes_accessed=2 * 10**6, transcendentals=0),
        compiler_params=grant(16),
        name="field",
    )(arrived, near_hot, own_hot, density, jnp.asarray(shell_table()))
    returned = exchange(back)
    return pl.pallas_call(
        fiber_kernel,
        out_shape=shape(8, 256),
        scratch_shapes=[pltpu.VMEM((8, 256), F32)],
        cost_estimate=pl.CostEstimate(flops=10**8, bytes_accessed=2 * 10**6, transcendentals=0),
        compiler_params=grant(8),
        name="fiber",
    )(returned, slot, rank, tension.reshape(1, NODES), split)


def solution(mesh):
    both = ("aa", "ba")
    in_specs = (
        P(None, both), P(None, both), P(both), P(both), P(both, None, None), P(both, None, None),
        P(), P(both), P(both), P(both, None), P(both, None, None),
    )
    return jax.shard_map(
        local, mesh=mesh, in_specs=in_specs, out_specs=P(both, None), check_vma=False
    )
```
